32 devices in a mesh: lat: 4 (over y, x), lon: 8 (over z, core).
Axes of the slice: x: 2, y: 2, z: 4, core: 2. Of those that a mesh axis runs over, the one named last changes fastest.
Arguments:
- activations: bfloat16 [4, 16, 720, 512], P(None, 'lat', 'lon'), may hold values from -48 to 48
- upstream: bfloat16 [4, 16, 720, 512], P(None, 'lat', 'lon'), may hold values from -6 to 6
- master: float32 [512, 9, 512], P(('lat', 'lon')), may hold values from -0.09375 to 0.09375
- moment_one: float32 [512, 9, 512], P(('lat', 'lon')), may hold values from -2.5 to 2.5
- moment_two: float32 [512, 9, 512], P(('lat', 'lon')), may hold values from 0.01 to 1
Outputs:
- input_grad: bfloat16 [4, 16, 720, 512], P(None, 'lat', 'lon')
- new_weights: bfloat16 [512, 9, 512], replicated
- new_master: float32 [512, 9, 512], P(('lat', 'lon'))
- new_moment_one: float32 [512, 9, 512], P(('lat', 'lon'))
- new_moment_two: float32 [512, 9, 512], P(('lat', 'lon'))
- clipped_grad: float32 [512, 9, 512], P(('lat', 'lon'))
The draws below stay inside these ranges and needn't reach their ends.
All inputs are finite; a program needn't handle non-finite values.
Results may differ from the reference program's by a relative error of at most 0.0049.
Values may be sent and summed in bfloat16 or wider, within the bound.
A program may use at most 128 MiB of HBM per device.

```python
import math
import jax
import jax.numpy as jnp
from jax import lax

CIN = 512
COUT = 512
TAPS = 9
BATCH = 4
COLS_DEV = 90
NLAT = 16
NLON = 720
N_LON = 8


def draw_activations(key, part):
    key_noise, key_spread = jax.random.split(key, 2)
    key_pair = jax.random.fold_in(key, 77)
    channel_ramp = jnp.sqrt(1.0 + 2.0 * jnp.arange(CIN, dtype=jnp.float32) / CIN)
    spread = jnp.exp(jax.random.uniform(key_spread, (CIN,), jnp.float32, 0.0, jnp.log(10.0)))
    chan_scale = channel_ramp * spread / 4.0
    pairing = jax.random.permutation(key_pair, N_LON)
    col_block = jnp.arange(NLON, dtype=jnp.int32) // COLS_DEV
    chan_block = jnp.arange(CIN, dtype=jnp.int32) // (CIN // N_LON)
    heavy = pairing[col_block][:, None] == chan_block[None, :]
    boost = jnp.where(heavy, 6.0, 1.0).astype(jnp.float32)[None, None, :, :]
    noise_draw = jax.random.normal(key_noise, (BATCH, NLAT, NLON, CIN), jnp.float32)
    values = noise_draw * chan_scale * boost
    return jnp.clip(values, -48.0, 48.0).astype(jnp.bfloat16)


def level_of(key, dims, cuts, low, top_value):
    factor_of = 1.0
    for dim, parts in cuts:
        draws = jax.random.uniform(jax.random.fold_in(jax.random.fold_in(key, 6), dim), (parts,), jnp.float32, low / len(cuts), top_value / len(cuts))
        factor_of = factor_of * jnp.repeat(jnp.exp(draws), dims[dim] // parts).reshape((-1,) + (1,) * (len(dims) - 1 - dim))
    return factor_of


def scatter_about(stream_key, extent, deviation, limit, cuts=(), kind=jnp.bfloat16):
    level = level_of(stream_key, extent, cuts, -0.22, 0.18) if cuts else 1.0
    result = jax.random.normal(stream_key, extent, jnp.float32) * deviation * level
    return jnp.minimum(jnp.maximum(result, -limit), limit).astype(kind)


def setup_inputs(seed: int = 0) -> dict:
    key_list = jax.random.split(jax.random.key(seed), 6)
    activations = draw_activations(jax.random.fold_in(key_list[5], 71), 0)
    upstream = scatter_about(key_list[1], (BATCH, NLAT, NLON, COUT), 1.0, 6.0, ((1, 4), (2, 8)))
    master = scatter_about(key_list[2], (CIN, TAPS, COUT), (CIN * TAPS) ** -0.5, 0.09375, ((0, 32),), jnp.float32)
    moment_one = scatter_about(key_list[3], (CIN, TAPS, COUT), 0.3, 2.5, ((0, 32),), jnp.float32)
    moment_two = jnp.clip(jnp.exp(math.log(1.0) - 4.6051702 * jax.random.uniform(key_list[4], (CIN, TAPS, COUT), jnp.float32) ** level_of(key_list[4], (CIN, TAPS, COUT), ((0, 32),), -0.2, 0.2)), 0.01, 1.0)
    return {"activations": activations, "upstream": upstream, "master": master, "moment_one": moment_one, "moment_two": moment_two}


learn_rate = 0.01
beta_one = 0.9
beta_two = 0.999
adam_eps = 1e-08
decay_rate = 0.1
step_count = 10.0
norm_eps = 1e-06

def widen_field(field):
    padded = jnp.pad(field, ((1, 1), (0, 0), (0, 0)))
    return jnp.concatenate([padded[:, -1:, :], padded, padded[:, :1, :]], axis=1)

def reference(activations, upstream, master, moment_one, moment_two):
    weights = master.astype(jnp.bfloat16)

    def one_sample(grad_total, sample):
        act_one, up_one = sample
        act_wide = widen_field(act_one)
        up_wide = widen_field(up_one)
        up_flat = up_one.reshape(-1, COUT)
        data_sum = jnp.zeros((NLAT * NLON, CIN), jnp.float32)
        tap_parts = []
        for tap_index in range(9):
            row_off, col_off = divmod(tap_index, 3)
            shifted = up_wide[2 - row_off:2 - row_off + NLAT, 2 - col_off:2 - col_off + NLON, :].reshape(-1, COUT)
            data_sum = data_sum + jnp.dot(shifted, weights[:, tap_index, :].T, preferred_element_type=jnp.float32)
            act_tap = act_wide[row_off:row_off + NLAT, col_off:col_off + NLON, :].reshape(-1, CIN)
            tap_parts.append(jnp.dot(act_tap.T, up_flat, preferred_element_type=jnp.float32))
        grad_total = grad_total + jnp.stack(tap_parts, axis=1)
        return (grad_total, data_sum.reshape(NLAT, NLON, CIN).astype(jnp.bfloat16))
    grad_total, input_grad = lax.scan(one_sample, jnp.zeros((CIN, 9, COUT), jnp.float32), (activations, upstream))
    max_norm = math.sqrt(float(CIN * TAPS * COUT))
    square_sum = jnp.sum(grad_total * grad_total)
    clip_factor = jnp.minimum(1.0, max_norm / (jnp.sqrt(square_sum) + norm_eps))
    grad_scaled = clip_factor * grad_total
    new_one = beta_one * moment_one + (1.0 - beta_one) * grad_scaled
    new_two = beta_two * moment_two + (1.0 - beta_two) * grad_scaled * grad_scaled
    first_hat = new_one / (1.0 - beta_one ** step_count)
    second_hat = new_two / (1.0 - beta_two ** step_count)
    new_master = master - learn_rate * (first_hat / (jnp.sqrt(second_hat) + adam_eps) + decay_rate * master)
    new_weights = new_master.astype(jnp.bfloat16)
    return (input_grad, new_weights, new_master, new_one, new_two, grad_scaled)
```

```python
import functools
import math

import jax
import jax.numpy as jnp
from jax import lax
from jax.experimental import pallas as pl
from jax.experimental.pallas import tpu as pltpu
from jax.sharding import PartitionSpec as P

MESH = pl.DeviceIdType.MESH

CIN = 512
COUT = 512
TAPS = 9


learn_rate = 0.01
beta_one = 0.9
beta_two = 0.999
adam_eps = 1e-08
decay_rate = 0.1
step_count = 10.0
norm_eps = 1e-06


def halo_kernel(n_lat, n_lon, *refs):
    sources, landings, (send_sem, recv_sem) = refs[:8], refs[8:16], refs[16:]
    lat, lon = lax.axis_index("lat"), lax.axis_index("lon")
    steps = ((-1, 0), (1, 0), (0, -1), (0, 1), (-1, -1), (-1, 1), (1, -1), (1, 1))
    targets = [
        (lax.rem(lat + dy + n_lat, n_lat), lax.rem(lon + dx + n_lon, n_lon)) for dy, dx in steps
    ]
    barrier = pltpu.get_barrier_semaphore()
    for target in targets:
        pl.semaphore_signal(barrier, inc=1, device_id=target, device_id_type=MESH)
    pl.semaphore_wait(barrier, len(targets))
    copies = []
    for index, target in enumerate(targets):
        copy = pltpu.make_async_remote_copy(
            src_ref=sources[index], dst_ref=landings[index], send_sem=send_sem.at[index],
            recv_sem=recv_sem.at[index], device_id=target, device_id_type=MESH,
        )
        copy.start()
        copies.append(copy)
    for copy in copies:
        copy.wait()


def widened(fields):
    both = jnp.stack(fields)
    top, bottom = both[:, :, 0], both[:, :, -1]
    pieces = (
        top, bottom, both[:, :, :, 0], both[:, :, :, -1],
        top[:, :, 0], top[:, :, -1], bottom[:, :, 0], bottom[:, :, -1],
    )
    landed = pl.pallas_call(
        functools.partial(halo_kernel, lax.axis_size("lat"), lax.axis_size("lon")),
        out_shape=tuple(jax.ShapeDtypeStruct(p.shape, p.dtype) for p in pieces),
        in_specs=[pl.BlockSpec(memory_space=pltpu.VMEM)] * 8,
        out_specs=(pl.BlockSpec(memory_space=pltpu.VMEM),) * 8,
        scratch_shapes=[pltpu.SemaphoreType.DMA((8,)), pltpu.SemaphoreType.DMA((8,))],
        compiler_params=pltpu.CompilerParams(
            collective_id=1, has_side_effects=True, vmem_limit_bytes=24 * 1024 * 1024
        ),
        name="halo",
    )(*pieces)
    below, above, east, west, below_east, below_west, above_east, above_west = landed

    def row(start, middle, end):
        return jnp.concatenate([start[:, None, None], middle[:, None], end[:, None, None]], axis=2)

    wide = []
    for index, field in enumerate(fields):
        middle = jnp.concatenate(
            [west[index][:, :, None], field, east[index][:, :, None]], axis=2
        )
        first = row(above_west[index], above[index], above_east[index])
        last = row(below_west[index], below[index], below_east[index])
        wide.append(mask_poles(jnp.concatenate([first, middle, last], axis=1)))
    return wide


def mask_poles(wide_field):
    lat_index = lax.axis_index("lat")
    lat_count = lax.axis_size("lat")
    total_rows = wide_field.shape[1]
    row_ids = lax.broadcasted_iota(jnp.int32, (1, total_rows, 1, 1), 1)
    upper = jnp.logical_and(row_ids == 0, lat_index == 0)
    lower = jnp.logical_and(row_ids == total_rows - 1, lat_index == lat_count - 1)
    return jnp.where(jnp.logical_or(upper, lower), jnp.zeros((), wide_field.dtype), wide_field)


def input_taps(act_wide, grad_flat, lat_rows, lon_cols):

    def input_compute(first_row, row_count):
        tap_parts = []
        for tap_index in range(9):
            row_off, col_off = divmod(tap_index, 3)
            tap_slab = act_wide[
                :, row_off : row_off + lat_rows, col_off : col_off + lon_cols, :
            ].reshape(-1, row_count)
            tap_parts.append(
                lax.dot_general(
                    tap_slab,
                    grad_flat,
                    (((0,), (0,)), ((), ())),
                    preferred_element_type=jnp.float32,
                )
            )
        return jnp.stack(tap_parts, axis=1)

    return input_compute


def reduce_update_gather(
    n_lat, n_q, max_norm, part, master, one, two,
    gathered, new_master, new_one, new_two, clipped,
    core_in, sums, right_in, left_in, lat_out, lat_in, norm_out, norm_in,
    send_sem, recv_sem,
):
    lat = lax.axis_index("lat")
    lon = lax.axis_index("lon")
    core = lax.rem(lon, 2)
    q = lon // 2
    hops = n_q // 2
    half = n_lat // 2
    counter = [0]
    pending = []

    def at(lat_id, q_id, core_id):
        return (lat_id, q_id * 2 + core_id)

    partner = at(lat, q, 1 - core)
    right_q = lax.rem(q + 1, n_q)
    left_q = lax.rem(q + n_q - 1, n_q)
    right, left = at(lat, right_q, core), at(lat, left_q, core)
    q_peers = [at(lat, lax.rem(q + d, n_q), core) for d in range(1, n_q)]
    lat_peers = [at(lax.rem(lat + d, n_lat), q, core) for d in range(1, n_lat)]

    def send(src, dst, target):
        index = counter[0]
        counter[0] += 1
        copy = pltpu.make_async_remote_copy(
            src_ref=src, dst_ref=dst, send_sem=send_sem.at[index],
            recv_sem=recv_sem.at[index], device_id=target, device_id_type=MESH,
        )
        copy.start()
        pending.append(copy)
        return copy

    def wrap(index, size):
        return lax.rem(index + size, size)

    barrier = pltpu.get_barrier_semaphore()
    greeted = [partner] + q_peers + lat_peers
    for device in greeted:
        pl.semaphore_signal(barrier, inc=1, device_id=device, device_id_type=MESH)
    pl.semaphore_wait(barrier, len(greeted))

    order = []
    for step in range(hops):
        for block in (hops - step, -hops + step):
            if block % n_q not in order:
                order.append(block % n_q)
    order.append(0)
    core_copies = []
    for offset in order:
        block = lax.rem(q + offset, n_q)
        core_copies.append(
            send(part.at[:, :, block, 1 - core], core_in.at[:, :, block], partner)
        )
    arrived = {}

    def core_sum(offset):
        if offset in arrived:
            return
        arrived[offset] = True
        core_copies[order.index(offset)].wait_recv()
        block = lax.rem(q + offset, n_q)

        @pl.loop(0, n_lat)
        def _(row):
            sums[block, row] = (
                part[:, row, block, core] + core_in[:, row, block]
            ).astype(jnp.bfloat16)

    def add_into(block, low, high, source):
        @pl.loop(low, high)
        def _(row):
            sums[block, row] = (
                sums[block, row].astype(jnp.float32) + source[row].astype(jnp.float32)
            ).astype(jnp.bfloat16)

    ring = []
    for step in range(hops):
        right_off = (hops - step) % n_q
        left_off = (step - hops) % n_q
        core_sum(right_off)
        core_sum(left_off)
        right_block = lax.rem(q + right_off, n_q)
        left_block = lax.rem(q + left_off, n_q)
        if step == 0:
            ring.append((
                send(sums.at[right_block, pl.ds(0, half)], right_in.at[0, pl.ds(0, half)], right),
                send(sums.at[left_block, pl.ds(half, n_lat - half)],
                     left_in.at[0, pl.ds(half, n_lat - half)], left),
            ))
        else:
            from_left, from_right = ring[-1]
            bounds = (0, half, half, n_lat) if step == 1 else (0, n_lat, 0, n_lat)
            from_left.wait_recv()
            add_into(right_block, bounds[0], bounds[1], right_in.at[step - 1])
            going_right = send(sums.at[right_block], right_in.at[step], right)
            from_right.wait_recv()
            add_into(left_block, bounds[2], bounds[3], left_in.at[step - 1])
            ring.append((going_right, send(sums.at[left_block], left_in.at[step], left)))
    core_sum(0)
    for copy in ring[-1]:
        copy.wait_recv()

    def q_total(row):
        total = part[:, row, q, core] + core_in[:, row, q]
        if hops > 1:
            return (
                total + right_in[hops - 1, row].astype(jnp.float32)
                + left_in[hops - 1, row].astype(jnp.float32)
            )
        return total + jnp.where(
            row < half, right_in[0, row].astype(jnp.float32), left_in[0, row].astype(jnp.float32)
        )

    lat_copies = []
    for step in range(1, n_lat):
        target = lax.rem(lat + step, n_lat)
        lat_out[step - 1] = q_total(target).astype(jnp.bfloat16)
        lat_copies.append(send(lat_out.at[step - 1], lat_in.at[step - 1], lat_peers[step - 1]))
    grad = q_total(lat)
    for step, copy in enumerate(lat_copies):
        copy.wait_recv()
        grad = grad + lat_in[step].astype(jnp.float32)
    clipped[...] = grad

    square = jnp.sum(grad * grad)
    slot = 0
    for stage, peers in enumerate(([partner], q_peers, lat_peers)):
        norm_out[stage] = jnp.full(norm_out.shape[1:], square, jnp.float32)
        copies = []
        for target in peers:
            copies.append(send(norm_out.at[stage], norm_in.at[slot], target))
            slot += 1
        tile = norm_out[stage]
        for index, copy in enumerate(copies):
            copy.wait_recv()
            tile = tile + norm_in[slot - len(peers) + index]
        square = jnp.max(tile)
    square = jnp.full((1, 1), square, jnp.float32)
    clip_factor = jnp.minimum(1.0, max_norm / (jnp.sqrt(square) + norm_eps))

    @pl.loop(0, clipped.shape[0])
    def _(tap):
        scaled = clip_factor * clipped[tap]
        clipped[tap] = scaled
        first = beta_one * one[tap] + (1.0 - beta_one) * scaled
        second = beta_two * two[tap] + (1.0 - beta_two) * scaled * scaled
        new_one[tap] = first
        new_two[tap] = second
        first_hat = first / (1.0 - beta_one**step_count)
        second_hat = second / (1.0 - beta_two**step_count)
        updated = master[tap] - learn_rate * (
            first_hat / (jnp.sqrt(second_hat) + adam_eps) + decay_rate * master[tap]
        )
        new_master[tap] = updated
        gathered[core, q, lat, tap] = updated.astype(jnp.bfloat16)

    copies = [
        send(gathered.at[core, q, lat], gathered.at[core, q, lat], peer) for peer in lat_peers
    ]
    for copy in copies:
        copy.wait_recv()
    core_in_copies = []

    def to_partner(block, low, count):
        piece = gathered.at[core, block, pl.ds(low, count)]
        core_in_copies.append(send(piece, piece, partner))

    from_left = from_right = None
    for step in range(hops):
        last = step == hops - 1
        right_block = wrap(q - step, n_q)
        left_block = lax.rem(q + step, n_q)
        if from_left is not None:
            from_left.wait_recv()
        piece = gathered.at[core, right_block, pl.ds(0, half if last else n_lat)]
        going_right = send(piece, piece, right)
        if from_right is not None:
            from_right.wait_recv()
        low = half if last else 0
        piece = gathered.at[core, left_block, pl.ds(low, n_lat - low)]
        going_left = send(piece, piece, left)
        to_partner(right_block, 0, n_lat)
        if step > 0:
            to_partner(left_block, 0, n_lat)
        from_left, from_right = going_right, going_left
    far = lax.rem(q + hops, n_q)
    from_left.wait_recv()
    to_partner(far, 0, half)
    from_right.wait_recv()
    to_partner(far, half, n_lat - half)
    for copy in core_in_copies:
        copy.wait_recv()
    for copy in pending:
        copy.wait_send()


def fused_update(partial, master, one, two):
    n_lat, n_q = lax.axis_size("lat"), lax.axis_size("lon") // 2
    taps, rows, width = master.shape
    part = partial.reshape(taps, n_lat, n_q, 2, rows, width)
    max_norm = math.sqrt(float(partial.size))
    shard = jax.ShapeDtypeStruct(master.shape, jnp.float32)
    hops = n_q // 2
    half_type = jnp.bfloat16
    block = (n_lat, taps, rows, width)
    peers = n_q + n_lat - 1
    vmem = pl.BlockSpec(memory_space=pltpu.VMEM)
    copies = 64 + 8 * (n_q + n_lat)
    return pl.pallas_call(
        functools.partial(reduce_update_gather, n_lat, n_q, max_norm),
        out_shape=(
            jax.ShapeDtypeStruct((2, n_q) + block, half_type), shard, shard, shard, shard,
        ),
        in_specs=[vmem] * 4,
        out_specs=(vmem,) * 5,
        scratch_shapes=[
            pltpu.VMEM((taps, n_lat, n_q, rows, width), jnp.float32),
            pltpu.VMEM((n_q,) + block, half_type),
            pltpu.VMEM((hops,) + block, half_type),
            pltpu.VMEM((hops,) + block, half_type),
            pltpu.VMEM((n_lat - 1, taps, rows, width), half_type),
            pltpu.VMEM((n_lat - 1, taps, rows, width), half_type),
            pltpu.VMEM((3, 8, 128), jnp.float32),
            pltpu.VMEM((peers, 8, 128), jnp.float32),
            pltpu.SemaphoreType.DMA((copies,)),
            pltpu.SemaphoreType.DMA((copies,)),
        ],
        compiler_params=pltpu.CompilerParams(
            collective_id=0, has_side_effects=True, vmem_limit_bytes=60 * 1024 * 1024
        ),
        name="reduce_update_gather",
    )(part, master, one, two)


LANE_TILE = 128
ROW_TILE = 16


def selector(shape, rows_of):
    rows = lax.broadcasted_iota(jnp.int32, shape, 0)
    cols = lax.broadcasted_iota(jnp.int32, shape, 1)
    return jnp.where(rows_of(rows, cols), 1.0, 0.0).astype(jnp.bfloat16)


def whole_step(
    n_lat, n_q, max_norm, batch, lat_rows,
    up, act, master, one, two,
    input_grad, w_new, new_master, new_one, new_two, clipped,
    fields, halo_out, halo_in, w_old, part, core_in, mine,
    first_x, first_y, first_x_in, first_y_in, keep_x, keep_y,
    second_x, second_y, second_x_in, second_y_in, last_out, last_in,
    norm_out, norm_in, send_sem, recv_sem,
):
    lat = lax.axis_index("lat")
    lon = lax.axis_index("lon")
    n_lon = n_q * 2
    core = lax.rem(lon, 2)
    q = lon // 2
    taps, rows, width = master.shape
    cols = up.shape[0]
    group_rows = batch * lat_rows
    chunks, halo_rows = halo_out.shape[1], halo_out.shape[2]
    chunk = cols // chunks
    half = width // 2
    counter = [0]
    pending = []

    def at(lat_id, q_id, core_id):
        return (lat_id, q_id * 2 + core_id)

    x_lat = lat + 1 - 2 * lax.rem(lat, 2)
    y_lat = lax.rem(lat + 2, 4)
    d_lat = x_lat + y_lat - lat
    partner = at(lat, q, 1 - core)
    x_peer, y_peer, d_peer = at(x_lat, q, core), at(y_lat, q, core), at(d_lat, q, core)

    def across(k):
        flipped = q
        bit = 1
        while bit < n_q:
            if k & bit:
                flipped = flipped + bit - 2 * bit * lax.rem(flipped // bit, 2)
            bit *= 2
        return flipped

    z_ids = [across(k) for k in range(n_q)]
    z_peers = [at(lat, z_ids[k], core) for k in range(1, n_q)]
    west = (lat, lax.rem(lon + n_lon - 1, n_lon))
    east = (lat, lax.rem(lon + 1, n_lon))
    above = (jnp.maximum(lat - 1, 0), lon)
    below = (jnp.minimum(lat + 1, n_lat - 1), lon)

    def slots(count):
        start = counter[0]
        counter[0] += count
        return start

    def remote(src, dst, target, index):
        return pltpu.make_async_remote_copy(
            src_ref=src, dst_ref=dst, send_sem=send_sem.at[index],
            recv_sem=recv_sem.at[index], device_id=target, device_id_type=MESH,
        )

    def send(src, dst, target):
        copy = remote(src, dst, target, slots(1))
        copy.start()
        pending.append(copy)
        return copy

    barrier = pltpu.get_barrier_semaphore()
    other_west = lax.rem(q + n_q - 1, n_q) * 2 + 1
    other_east = lax.rem(q + 1, n_q) * 2
    outside = (lat, jnp.where(core == 0, other_west, other_east))
    greeted = [partner, outside, x_peer, y_peer, d_peer] + z_peers
    for device in greeted:
        pl.semaphore_signal(barrier, inc=1, device_id=device, device_id_type=MESH)

    for tap in range(taps):
        w_old[tap, lat, q, core] = master[tap].astype(jnp.bfloat16)

    @pl.loop(0, cols)
    def _(j):
        fields[1, j + 1] = up[j]

    def last_row(index):
        return lax.rem(index, lat_rows) == lat_rows - 1

    def first_row(index):
        return lax.rem(index, lat_rows) == 0

    span = chunk * group_rows
    picked = chunk * batch
    take = [
        selector((halo_rows, span), lambda m, n: n == m * lat_rows),
        selector((halo_rows, span), lambda m, n: n == m * lat_rows + lat_rows - 1),
    ]

    @pl.loop(0, chunks)
    def _(c):
        block = up[pl.ds(c * chunk, chunk)].reshape(span, width)
        for side in range(2):
            halo_out[side, c] = jnp.dot(
                take[side], block, preferred_element_type=jnp.float32
            ).astype(jnp.bfloat16)

    pl.semaphore_wait(barrier, len(greeted))

    class Gather:
        def __init__(self, buffer, cut):
            self.buffer, self.cut = buffer, cut
            self.to_z, self.to_x, self.to_y, self.to_core = {}, {}, {}, []
            self.diag_x, self.diag_y = {}, {}

        def block(self, lat_id, q_id, low, high):
            return self.buffer.at[:, lat_id, q_id, core, :, pl.ds(low, high - low)]

        def give(self, lat_id, q_id, low, high, target):
            piece = self.block(lat_id, q_id, low, high)
            return send(piece, piece, target)

        def spread(self, k):
            self.to_x[k] = self.give(lat, z_ids[k], 0, width, x_peer)
            self.to_y[k] = self.give(lat, z_ids[k], 0, width, y_peer)
            self.to_core.append(self.give(lat, z_ids[k], 0, width, partner))

        def start_z(self):
            for k in range(1, n_q):
                self.to_z[k] = self.give(lat, q, 0, width, z_peers[k - 1])

        def start(self):
            self.start_z()
            self.spread(0)

        def from_z(self, k):
            self.to_z[k].wait_recv()
            self.spread(k)

        def relay(self, k):
            self.to_x[k].wait_recv()
            self.diag_y[k] = self.give(x_lat, z_ids[k], 0, self.cut, y_peer)
            self.to_core.append(self.give(x_lat, z_ids[k], 0, width, partner))
            self.to_y[k].wait_recv()
            if self.cut < width:
                self.diag_x[k] = self.give(y_lat, z_ids[k], self.cut, width, x_peer)
            self.to_core.append(self.give(y_lat, z_ids[k], 0, width, partner))

        def close(self, k):
            self.diag_y[k].wait_recv()
            self.to_core.append(self.give(d_lat, z_ids[k], 0, self.cut, partner))
            if self.cut < width:
                self.diag_x[k].wait_recv()
                self.to_core.append(self.give(d_lat, z_ids[k], self.cut, width, partner))

        def finish(self):
            for copy in self.to_core:
                copy.wait_recv()

    old = Gather(w_old, width)
    old.start_z()

    up_slot, down_slot = slots(1), slots(1)
    to_above = remote(halo_out.at[0], halo_in.at[0], above, up_slot)
    to_below = remote(halo_out.at[1], halo_in.at[1], below, down_slot)
    has_above, has_below = lat > 0, lat < n_lat - 1

    @pl.when(has_above)
    def _():
        to_above.start()

    @pl.when(has_below)
    def _():
        to_below.start()

    def edges(field):
        to_west = send(fields.at[field, 1], fields.at[field, cols + 1], west)
        to_east = send(fields.at[field, cols], fields.at[field, 0], east)
        return to_west, to_east

    middle_edges = edges(1)
    old.spread(0)

    acts = act[...].reshape(cols * group_rows, width)
    part_slot = slots(taps)

    def part_copy(tap):
        return remote(
            part.at[tap, :, :, 1 - core], core_in.at[tap], partner, part_slot + tap
        )

    def weight_taps(group):
        @pl.loop(0, 3)
        def _(s):
            shifted = fields[group, pl.ds(2 - s, cols)].reshape(cols * group_rows, width)
            tap = group * 3 + s
            part[tap] = lax.dot_general(
                acts, shifted, (((0,), (0,)), ((), ())), preferred_element_type=jnp.float32
            ).reshape(n_lat, n_q, 2, rows, width)
            part_copy(tap).start()

    first, second, third = {}, {}, {}

    def reduce_first(group):
        @pl.loop(0, 3)
        def _(s):
            tap = group * 3 + s
            part_copy(tap).wait_recv()
            for k in range(n_q):
                def total(lat_id):
                    return part[tap, lat_id, k, core] + core_in[tap, lat_id, k]

                mine[tap, k] = total(lat)
                value = total(x_lat)
                keep_x[tap, k] = value[:, :half]
                first_x[tap, 0, k] = value[:, half:].astype(jnp.bfloat16)
                value = total(y_lat)
                first_y[tap, 0, k] = value[:, :half].astype(jnp.bfloat16)
                keep_y[tap, k] = value[:, half:]
                value = total(d_lat)
                first_y[tap, 1, k] = value[:, :half].astype(jnp.bfloat16)
                first_x[tap, 1, k] = value[:, half:].astype(jnp.bfloat16)

        piece = pl.ds(group * 3, 3)
        first[group] = (
            send(first_x.at[piece], first_x_in.at[piece], x_peer),
            send(first_y.at[piece], first_y_in.at[piece], y_peer),
        )

    def reduce_second(group):
        piece = pl.ds(group * 3, 3)
        for copy in first[group]:
            copy.wait_recv()

        @pl.loop(0, 3)
        def _(s):
            tap = group * 3 + s
            for k in range(n_q):
                second_x[tap, k] = (
                    keep_x[tap, k] + first_y_in[tap, 1, k].astype(jnp.float32)
                ).astype(jnp.bfloat16)
                second_y[tap, k] = (
                    keep_y[tap, k] + first_x_in[tap, 1, k].astype(jnp.float32)
                ).astype(jnp.bfloat16)

        second[group] = (
            send(second_x.at[piece], second_x_in.at[piece], x_peer),
            send(second_y.at[piece], second_y_in.at[piece], y_peer),
        )

    def reduce_third(group):
        piece = pl.ds(group * 3, 3)
        for copy in second[group]:
            copy.wait_recv()

        @pl.loop(0, 3)
        def _(s):
            tap = group * 3 + s
            for k in range(n_q):
                low = (
                    mine[tap, k, :, :half] + first_y_in[tap, 0, k].astype(jnp.float32)
                    + second_x_in[tap, k].astype(jnp.float32)
                )
                high = (
                    mine[tap, k, :, half:] + first_x_in[tap, 0, k].astype(jnp.float32)
                    + second_y_in[tap, k].astype(jnp.float32)
                )
                mine[tap, k, :, :half] = low
                mine[tap, k, :, half:] = high
            for k in range(1, n_q):
                last_out[k - 1, tap] = mine[tap, z_ids[k]].astype(jnp.bfloat16)

        third[group] = [
            send(last_out.at[k - 1, piece], last_in.at[k - 1, piece], z_peers[k - 1])
            for k in range(1, n_q)
        ]

    for copy in middle_edges:
        copy.wait_recv()
    weight_taps(1)
    for k in range(1, n_q):
        old.from_z(k)
    reduce_first(1)

    @pl.when(has_below)
    def _():
        to_above.wait_recv()

    @pl.when(has_above)
    def _():
        to_below.wait_recv()

    @pl.when(jnp.logical_not(has_below))
    def _():
        halo_in[0] = jnp.zeros(halo_in.shape[1:], halo_in.dtype)

    @pl.when(jnp.logical_not(has_above))
    def _():
        halo_in[1] = jnp.zeros(halo_in.shape[1:], halo_in.dtype)

    shift = [
        selector((span, span), lambda m, n: jnp.logical_and(n == m + 1, jnp.logical_not(last_row(m)))),
        selector((span, span), lambda m, n: jnp.logical_and(n == m - 1, jnp.logical_not(first_row(m)))),
    ]
    place = [
        selector((span, halo_rows), lambda m, n: jnp.logical_and(n == m // lat_rows, last_row(m))),
        selector((span, halo_rows), lambda m, n: jnp.logical_and(n == m // lat_rows, first_row(m))),
    ]

    @pl.loop(0, chunks)
    def _(c):
        block = up[pl.ds(c * chunk, chunk)].reshape(span, width)
        for side in range(2):
            moved = jnp.dot(shift[side], block, preferred_element_type=jnp.float32)
            moved = moved + jnp.dot(
                place[side], halo_in[side, c], preferred_element_type=jnp.float32
            )
            fields[2 * side, pl.ds(1 + c * chunk, chunk)] = moved.astype(jnp.bfloat16).reshape(
                chunk, group_rows, width
            )

    upper_edges, lower_edges = edges(0), edges(2)
    for copy in upper_edges:
        copy.wait_recv()
    weight_taps(0)
    reduce_first(0)
    for k in range(n_q):
        old.relay(k)
    reduce_second(1)
    for copy in lower_edges:
        copy.wait_recv()
    weight_taps(2)
    reduce_first(2)
    reduce_second(0)
    reduce_third(1)
    for k in range(n_q):
        old.close(k)
    reduce_second(2)
    reduce_third(0)
    reduce_third(2)

    for group in range(3):
        for copy in third[group]:
            copy.wait_recv()
    grad_square = jnp.zeros((rows, width), jnp.float32)

    def finish_tap(tap, total):
        grad = mine[tap, q]
        for k in range(n_q - 1):
            grad = grad + last_in[k, tap].astype(jnp.float32)
        clipped[tap] = grad
        return total + grad * grad

    grad_square = lax.fori_loop(0, taps, finish_tap, grad_square)
    square = jnp.sum(grad_square)

    old.finish()
    piece_cols = cols // 2

    def input_piece(index):
        total = None
        for tap in range(taps):
            r, s = divmod(tap, 3)
            shifted = fields[r, pl.ds(index * piece_cols + 2 - s, piece_cols)]
            product = lax.dot_general(
                shifted.reshape(piece_cols * group_rows, width),
                w_old[tap].reshape(-1, width),
                (((1,), (1,)), ((), ())), preferred_element_type=jnp.float32,
            )
            total = product if total is None else total + product
        input_grad[pl.ds(index * piece_cols, piece_cols)] = total.astype(jnp.bfloat16).reshape(
            piece_cols, group_rows, width
        )

    slot = 0
    for stage, peers in enumerate(([partner], z_peers, [x_peer, y_peer, d_peer])):
        norm_out[stage] = jnp.full(norm_out.shape[1:], square, jnp.float32)
        copies = []
        for index, target in enumerate(peers):
            copies.append(send(norm_out.at[stage], norm_in.at[slot + index], target))
        tile = norm_out[stage]
        for index, copy in enumerate(copies):
            copy.wait_recv()
            tile = tile + norm_in[slot + index]
        slot += len(peers)
        square = jnp.max(tile)
    square = jnp.full((1, 1), square, jnp.float32)
    clip_factor = jnp.minimum(1.0, max_norm / (jnp.sqrt(square) + norm_eps))

    @pl.loop(0, taps)
    def _(tap):
        scaled = clip_factor * clipped[tap]
        clipped[tap] = scaled
        moment = beta_one * one[tap] + (1.0 - beta_one) * scaled
        spread = beta_two * two[tap] + (1.0 - beta_two) * scaled * scaled
        new_one[tap] = moment
        new_two[tap] = spread
        first_hat = moment / (1.0 - beta_one**step_count)
        second_hat = spread / (1.0 - beta_two**step_count)
        updated = master[tap] - learn_rate * (
            first_hat / (jnp.sqrt(second_hat) + adam_eps) + decay_rate * master[tap]
        )
        new_master[tap] = updated
        w_new[tap, lat, q, core] = updated.astype(jnp.bfloat16)

    new = Gather(w_new, half)
    new.start()
    input_piece(0)
    for k in range(1, n_q):
        new.from_z(k)
    for k in range(n_q):
        new.relay(k)
    input_piece(1)
    for k in range(n_q):
        new.close(k)
    new.finish()

    @pl.when(has_above)
    def _():
        to_above.wait_send()

    @pl.when(has_below)
    def _():
        to_below.wait_send()

    @pl.loop(0, taps)
    def _(tap):
        part_copy(tap).wait_send()

    for copy in pending:
        copy.wait_send()


def fused_step(up, act, master, one, two, batch, lat_rows):
    n_lat, n_q = lax.axis_size("lat"), lax.axis_size("lon") // 2
    taps, rows, width = master.shape
    cols, group_rows, _ = up.shape
    half = width // 2
    chunk = max(c for c in range(1, 17) if cols % c == 0)
    chunks = cols // chunk
    halo_rows = -(-chunk * batch // ROW_TILE) * ROW_TILE
    max_norm = math.sqrt(float(n_lat * n_q * 2 * taps * rows * width))
    bf16, f32 = jnp.bfloat16, jnp.float32
    shard = jax.ShapeDtypeStruct(master.shape, f32)
    whole = (taps, n_lat, n_q, 2, rows, width)
    side = (taps, n_q, rows, half)
    vmem = pl.BlockSpec(memory_space=pltpu.VMEM)
    peers = n_q + n_lat - 1
    copies = 128 + 16 * (n_q + n_lat)
    return pl.pallas_call(
        functools.partial(whole_step, n_lat, n_q, max_norm, batch, lat_rows),
        out_shape=(
            jax.ShapeDtypeStruct(up.shape, bf16), jax.ShapeDtypeStruct(whole, bf16),
            shard, shard, shard, shard,
        ),
        in_specs=[vmem] * 5,
        out_specs=(vmem,) * 6,
        scratch_shapes=[
            pltpu.VMEM((3, cols + 2, group_rows, width), bf16),
            pltpu.VMEM((2, chunks, halo_rows, width), bf16),
            pltpu.VMEM((2, chunks, halo_rows, width), bf16),
            pltpu.VMEM(whole, bf16),
            pltpu.VMEM(whole, f32),
            pltpu.VMEM((taps, n_lat, n_q, rows, width), f32),
            pltpu.VMEM((taps, n_q, rows, width), f32),
            pltpu.VMEM((taps, 2) + side[1:], bf16),
            pltpu.VMEM((taps, 2) + side[1:], bf16),
            pltpu.VMEM((taps, 2) + side[1:], bf16),
            pltpu.VMEM((taps, 2) + side[1:], bf16),
            pltpu.VMEM(side, f32),
            pltpu.VMEM(side, f32),
            pltpu.VMEM(side, bf16),
            pltpu.VMEM(side, bf16),
            pltpu.VMEM(side, bf16),
            pltpu.VMEM(side, bf16),
            pltpu.VMEM((n_q - 1, taps, rows, width), bf16),
            pltpu.VMEM((n_q - 1, taps, rows, width), bf16),
            pltpu.VMEM((3, 8, LANE_TILE), f32),
            pltpu.VMEM((peers, 8, LANE_TILE), f32),
            pltpu.SemaphoreType.DMA((copies,)),
            pltpu.SemaphoreType.DMA((copies,)),
        ],
        compiler_params=pltpu.CompilerParams(
            collective_id=2, has_side_effects=True, vmem_limit_bytes=62 * 1024 * 1024
        ),
        name="whole_step",
    )(up, act, master, one, two)


def takes_fused(activations, master):
    n_lat, n_q = lax.axis_size("lat"), lax.axis_size("lon") // 2
    batch, lat_rows, cols, _ = activations.shape
    return (
        n_lat == 4 and n_q & (n_q - 1) == 0 and n_q > 1 and master.shape[0] % ROW_TILE == 0
        and (batch * lat_rows) % ROW_TILE == 0 and cols % 2 == 0
        and master.shape[2] % (2 * LANE_TILE) == 0 and master.shape[1] == 9
    )


def per_device(activations, upstream, master, moment_one, moment_two):
    if not takes_fused(activations, master):
        return per_device_general(activations, upstream, master, moment_one, moment_two)
    batch, lat_rows, cols, width = activations.shape

    def by_col(field):
        return jnp.transpose(field, (2, 0, 1, 3)).reshape(cols, batch * lat_rows, width)

    def by_tap(array):
        return jnp.transpose(array, (1, 0, 2))

    input_grad, gathered, new_master, new_one, new_two, clipped = fused_step(
        by_col(upstream), by_col(activations), by_tap(master), by_tap(moment_one),
        by_tap(moment_two), batch, lat_rows,
    )
    input_grad = jnp.transpose(
        input_grad.reshape(cols, batch, lat_rows, width), (1, 2, 0, 3)
    )
    new_weights = by_tap(gathered.reshape(gathered.shape[0], -1, gathered.shape[-1]))
    return (
        input_grad, new_weights, by_tap(new_master), by_tap(new_one), by_tap(new_two),
        by_tap(clipped),
    )


def per_device_general(activations, upstream, master, moment_one, moment_two):
    lat_rows = activations.shape[1]
    lon_cols = activations.shape[2]
    grad_flat = upstream.reshape(-1, upstream.shape[3])
    old_weights = master[:, ::-1].astype(jnp.bfloat16)
    old_full = lax.all_gather(old_weights, ("lat", "lon"), axis=0, tiled=True)
    act_wide, grad_wide = widened((activations, upstream))
    term_maker = input_taps(act_wide, grad_flat, lat_rows, lon_cols)
    partial = term_maker(jnp.int32(0), activations.shape[3])

    def by_tap(array):
        return jnp.transpose(array, (1, 0, 2))

    gathered, new_master, new_one, new_two, clipped = fused_update(
        by_tap(partial), by_tap(master), by_tap(moment_one), by_tap(moment_two)
    )
    new_weights = jnp.transpose(gathered, (2, 1, 0, 4, 3, 5)).reshape(
        activations.shape[3], gathered.shape[3], gathered.shape[5]
    )
    old_full, new_one = lax.optimization_barrier((old_full, new_one))
    input_grad = lax.conv_general_dilated(
        grad_wide,
        old_full.reshape(old_full.shape[0], 3, 3, old_full.shape[2]),
        (1, 1),
        "VALID",
        dimension_numbers=("NHWC", "OHWI", "NHWC"),
        preferred_element_type=jnp.float32,
    ).astype(jnp.bfloat16)
    return (
        input_grad, new_weights, by_tap(new_master), by_tap(new_one), by_tap(new_two),
        by_tap(clipped),
    )


def solution(mesh):
    in_specs = (
        P(None, "lat", "lon", None),
        P(None, "lat", "lon", None),
        P(("lat", "lon"), None, None),
        P(("lat", "lon"), None, None),
        P(("lat", "lon"), None, None),
    )
    out_specs = (
        P(None, "lat", "lon", None),
        P(),
        P(("lat", "lon"), None, None),
        P(("lat", "lon"), None, None),
        P(("lat", "lon"), None, None),
        P(("lat", "lon"), None, None),
    )
    return jax.shard_map(
        per_device, mesh=mesh, in_specs=in_specs, out_specs=out_specs, check_vma=False
    )
```

```python
import functools
import math

import jax
import jax.numpy as jnp
from jax import lax
from jax.experimental import pallas as pl
from jax.experimental.pallas import tpu as pltpu
from jax.sharding import PartitionSpec as P

MESH = pl.DeviceIdType.MESH

CIN = 512
COUT = 512
TAPS = 9


learn_rate = 0.01
beta_one = 0.9
beta_two = 0.999
adam_eps = 1e-08
decay_rate = 0.1
step_count = 10.0
norm_eps = 1e-06


def halo_kernel(n_lat, n_lon, *refs):
    sources, landings, (send_sem, recv_sem) = refs[:8], refs[8:16], refs[16:]
    lat, lon = lax.axis_index("lat"), lax.axis_index("lon")
    steps = ((-1, 0), (1, 0), (0, -1), (0, 1), (-1, -1), (-1, 1), (1, -1), (1, 1))
    targets = [
        (lax.rem(lat + dy + n_lat, n_lat), lax.rem(lon + dx + n_lon, n_lon)) for dy, dx in steps
    ]
    barrier = pltpu.get_barrier_semaphore()
    for target in targets:
        pl.semaphore_signal(barrier, inc=1, device_id=target, device_id_type=MESH)
    pl.semaphore_wait(barrier, len(targets))
    copies = []
    for index, target in enumerate(targets):
        copy = pltpu.make_async_remote_copy(
            src_ref=sources[index], dst_ref=landings[index], send_sem=send_sem.at[index],
            recv_sem=recv_sem.at[index], device_id=target, device_id_type=MESH,
        )
        copy.start()
        copies.append(copy)
    for copy in copies:
        copy.wait()


def widened(fields):
    both = jnp.stack(fields)
    top, bottom = both[:, :, 0], both[:, :, -1]
    pieces = (
        top, bottom, both[:, :, :, 0], both[:, :, :, -1],
        top[:, :, 0], top[:, :, -1], bottom[:, :, 0], bottom[:, :, -1],
    )
    landed = pl.pallas_call(
        functools.partial(halo_kernel, lax.axis_size("lat"), lax.axis_size("lon")),
        out_shape=tuple(jax.ShapeDtypeStruct(p.shape, p.dtype) for p in pieces),
        in_specs=[pl.BlockSpec(memory_space=pltpu.VMEM)] * 8,
        out_specs=(pl.BlockSpec(memory_space=pltpu.VMEM),) * 8,
        scratch_shapes=[pltpu.SemaphoreType.DMA((8,)), pltpu.SemaphoreType.DMA((8,))],
        compiler_params=pltpu.CompilerParams(
            collective_id=1, has_side_effects=True, vmem_limit_bytes=24 * 1024 * 1024
        ),
        name="halo",
    )(*pieces)
    below, above, east, west, below_east, below_west, above_east, above_west = landed

    def row(start, middle, end):
        return jnp.concatenate([start[:, None, None], middle[:, None], end[:, None, None]], axis=2)

    wide = []
    for index, field in enumerate(fields):
        middle = jnp.concatenate(
            [west[index][:, :, None], field, east[index][:, :, None]], axis=2
        )
        first = row(above_west[index], above[index], above_east[index])
        last = row(below_west[index], below[index], below_east[index])
        wide.append(mask_poles(jnp.concatenate([first, middle, last], axis=1)))
    return wide


def mask_poles(wide_field):
    lat_index = lax.axis_index("lat")
    lat_count = lax.axis_size("lat")
    total_rows = wide_field.shape[1]
    row_ids = lax.broadcasted_iota(jnp.int32, (1, total_rows, 1, 1), 1)
    upper = jnp.logical_and(row_ids == 0, lat_index == 0)
    lower = jnp.logical_and(row_ids == total_rows - 1, lat_index == lat_count - 1)
    return jnp.where(jnp.logical_or(upper, lower), jnp.zeros((), wide_field.dtype), wide_field)


def input_taps(act_wide, grad_flat, lat_rows, lon_cols):

    def input_compute(first_row, row_count):
        tap_parts = []
        for tap_index in range(9):
            row_off, col_off = divmod(tap_index, 3)
            tap_slab = act_wide[
                :, row_off : row_off + lat_rows, col_off : col_off + lon_cols, :
            ].reshape(-1, row_count)
            tap_parts.append(
                lax.dot_general(
                    tap_slab,
                    grad_flat,
                    (((0,), (0,)), ((), ())),
                    preferred_element_type=jnp.float32,
                )
            )
        return jnp.stack(tap_parts, axis=1)

    return input_compute


def reduce_update_gather(
    n_lat, n_q, max_norm, part, master, one, two,
    gathered, new_master, new_one, new_two, clipped,
    core_in, sums, right_in, left_in, lat_out, lat_in, norm_out, norm_in,
    send_sem, recv_sem,
):
    lat = lax.axis_index("lat")
    lon = lax.axis_index("lon")
    core = lax.rem(lon, 2)
    q = lon // 2
    hops = n_q // 2
    half = n_lat // 2
    counter = [0]
    pending = []

    def at(lat_id, q_id, core_id):
        return (lat_id, q_id * 2 + core_id)

    partner = at(lat, q, 1 - core)
    right_q = lax.rem(q + 1, n_q)
    left_q = lax.rem(q + n_q - 1, n_q)
    right, left = at(lat, right_q, core), at(lat, left_q, core)
    q_peers = [at(lat, lax.rem(q + d, n_q), core) for d in range(1, n_q)]
    lat_peers = [at(lax.rem(lat + d, n_lat), q, core) for d in range(1, n_lat)]

    def send(src, dst, target):
        index = counter[0]
        counter[0] += 1
        copy = pltpu.make_async_remote_copy(
            src_ref=src, dst_ref=dst, send_sem=send_sem.at[index],
            recv_sem=recv_sem.at[index], device_id=target, device_id_type=MESH,
        )
        copy.start()
        pending.append(copy)
        return copy

    def wrap(index, size):
        return lax.rem(index + size, size)

    barrier = pltpu.get_barrier_semaphore()
    greeted = [partner] + q_peers + lat_peers
    for device in greeted:
        pl.semaphore_signal(barrier, inc=1, device_id=device, device_id_type=MESH)
    pl.semaphore_wait(barrier, len(greeted))

    order = []
    for step in range(hops):
        for block in (hops - step, -hops + step):
            if block % n_q not in order:
                order.append(block % n_q)
    order.append(0)
    core_copies = []
    for offset in order:
        block = lax.rem(q + offset, n_q)
        core_copies.append(
            send(part.at[:, :, block, 1 - core], core_in.at[:, :, block], partner)
        )
    arrived = {}

    def core_sum(offset):
        if offset in arrived:
            return
        arrived[offset] = True
        core_copies[order.index(offset)].wait_recv()
        block = lax.rem(q + offset, n_q)

        @pl.loop(0, n_lat)
        def _(row):
            sums[block, row] = (
                part[:, row, block, core] + core_in[:, row, block]
            ).astype(jnp.bfloat16)

    def add_into(block, low, high, source):
        @pl.loop(low, high)
        def _(row):
            sums[block, row] = (
                sums[block, row].astype(jnp.float32) + source[row].astype(jnp.float32)
            ).astype(jnp.bfloat16)

    ring = []
    for step in range(hops):
        right_off = (hops - step) % n_q
        left_off = (step - hops) % n_q
        core_sum(right_off)
        core_sum(left_off)
        right_block = lax.rem(q + right_off, n_q)
        left_block = lax.rem(q + left_off, n_q)
        if step == 0:
            ring.append((
                send(sums.at[right_block, pl.ds(0, half)], right_in.at[0, pl.ds(0, half)], right),
                send(sums.at[left_block, pl.ds(half, n_lat - half)],
                     left_in.at[0, pl.ds(half, n_lat - half)], left),
            ))
        else:
            from_left, from_right = ring[-1]
            bounds = (0, half, half, n_lat) if step == 1 else (0, n_lat, 0, n_lat)
            from_left.wait_recv()
            add_into(right_block, bounds[0], bounds[1], right_in.at[step - 1])
            going_right = send(sums.at[right_block], right_in.at[step], right)
            from_right.wait_recv()
            add_into(left_block, bounds[2], bounds[3], left_in.at[step - 1])
            ring.append((going_right, send(sums.at[left_block], left_in.at[step], left)))
    core_sum(0)
    for copy in ring[-1]:
        copy.wait_recv()

    def q_total(row):
        total = part[:, row, q, core] + core_in[:, row, q]
        if hops > 1:
            return (
                total + right_in[hops - 1, row].astype(jnp.float32)
                + left_in[hops - 1, row].astype(jnp.float32)
            )
        return total + jnp.where(
            row < half, right_in[0, row].astype(jnp.float32), left_in[0, row].astype(jnp.float32)
        )

    lat_copies = []
    for step in range(1, n_lat):
        target = lax.rem(lat + step, n_lat)
        lat_out[step - 1] = q_total(target).astype(jnp.bfloat16)
        lat_copies.append(send(lat_out.at[step - 1], lat_in.at[step - 1], lat_peers[step - 1]))
    grad = q_total(lat)
    for step, copy in enumerate(lat_copies):
        copy.wait_recv()
        grad = grad + lat_in[step].astype(jnp.float32)
    clipped[...] = grad

    square = jnp.sum(grad * grad)
    slot = 0
    for stage, peers in enumerate(([partner], q_peers, lat_peers)):
        norm_out[stage] = jnp.full(norm_out.shape[1:], square, jnp.float32)
        copies = []
        for target in peers:
            copies.append(send(norm_out.at[stage], norm_in.at[slot], target))
            slot += 1
        tile = norm_out[stage]
        for index, copy in enumerate(copies):
            copy.wait_recv()
            tile = tile + norm_in[slot - len(peers) + index]
        square = jnp.max(tile)
    square = jnp.full((1, 1), square, jnp.float32)
    clip_factor = jnp.minimum(1.0, max_norm / (jnp.sqrt(square) + norm_eps))

    @pl.loop(0, clipped.shape[0])
    def _(tap):
        scaled = clip_factor * clipped[tap]
        clipped[tap] = scaled
        first = beta_one * one[tap] + (1.0 - beta_one) * scaled
        second = beta_two * two[tap] + (1.0 - beta_two) * scaled * scaled
        new_one[tap] = first
        new_two[tap] = second
        first_hat = first / (1.0 - beta_one**step_count)
        second_hat = second / (1.0 - beta_two**step_count)
        updated = master[tap] - learn_rate * (
            first_hat / (jnp.sqrt(second_hat) + adam_eps) + decay_rate * master[tap]
        )
        new_master[tap] = updated
        gathered[core, q, lat, tap] = updated.astype(jnp.bfloat16)

    copies = [
        send(gathered.at[core, q, lat], gathered.at[core, q, lat], peer) for peer in lat_peers
    ]
    for copy in copies:
        copy.wait_recv()
    core_in_copies = []

    def to_partner(block, low, count):
        piece = gathered.at[core, block, pl.ds(low, count)]
        core_in_copies.append(send(piece, piece, partner))

    from_left = from_right = None
    for step in range(hops):
        last = step == hops - 1
        right_block = wrap(q - step, n_q)
        left_block = lax.rem(q + step, n_q)
        if from_left is not None:
            from_left.wait_recv()
        piece = gathered.at[core, right_block, pl.ds(0, half if last else n_lat)]
        going_right = send(piece, piece, right)
        if from_right is not None:
            from_right.wait_recv()
        low = half if last else 0
        piece = gathered.at[core, left_block, pl.ds(low, n_lat - low)]
        going_left = send(piece, piece, left)
        to_partner(right_block, 0, n_lat)
        if step > 0:
            to_partner(left_block, 0, n_lat)
        from_left, from_right = going_right, going_left
    far = lax.rem(q + hops, n_q)
    from_left.wait_recv()
    to_partner(far, 0, half)
    from_right.wait_recv()
    to_partner(far, half, n_lat - half)
    for copy in core_in_copies:
        copy.wait_recv()
    for copy in pending:
        copy.wait_send()


def fused_update(partial, master, one, two):
    n_lat, n_q = lax.axis_size("lat"), lax.axis_size("lon") // 2
    taps, rows, width = master.shape
    part = partial.reshape(taps, n_lat, n_q, 2, rows, width)
    max_norm = math.sqrt(float(partial.size))
    shard = jax.ShapeDtypeStruct(master.shape, jnp.float32)
    hops = n_q // 2
    half_type = jnp.bfloat16
    block = (n_lat, taps, rows, width)
    peers = n_q + n_lat - 1
    vmem = pl.BlockSpec(memory_space=pltpu.VMEM)
    copies = 64 + 8 * (n_q + n_lat)
    return pl.pallas_call(
        functools.partial(reduce_update_gather, n_lat, n_q, max_norm),
        out_shape=(
            jax.ShapeDtypeStruct((2, n_q) + block, half_type), shard, shard, shard, shard,
        ),
        in_specs=[vmem] * 4,
        out_specs=(vmem,) * 5,
        scratch_shapes=[
            pltpu.VMEM((taps, n_lat, n_q, rows, width), jnp.float32),
            pltpu.VMEM((n_q,) + block, half_type),
            pltpu.VMEM((hops,) + block, half_type),
            pltpu.VMEM((hops,) + block, half_type),
            pltpu.VMEM((n_lat - 1, taps, rows, width), half_type),
            pltpu.VMEM((n_lat - 1, taps, rows, width), half_type),
            pltpu.VMEM((3, 8, 128), jnp.float32),
            pltpu.VMEM((peers, 8, 128), jnp.float32),
            pltpu.SemaphoreType.DMA((copies,)),
            pltpu.SemaphoreType.DMA((copies,)),
        ],
        compiler_params=pltpu.CompilerParams(
            collective_id=0, has_side_effects=True, vmem_limit_bytes=60 * 1024 * 1024
        ),
        name="reduce_update_gather",
    )(part, master, one, two)


LANE_TILE = 128
ROW_TILE = 16
OLD_LINE_TAPS = 6
NEW_LINE_TAPS = 2


def selector(shape, rows_of):
    rows = lax.broadcasted_iota(jnp.int32, shape, 0)
    cols = lax.broadcasted_iota(jnp.int32, shape, 1)
    return jnp.where(rows_of(rows, cols), 1.0, 0.0).astype(jnp.bfloat16)


def whole_step(
    n_lat, n_q, max_norm,
    up_hbm, act_hbm, master_hbm, one_hbm, two_hbm,
    input_grad, w_new, new_master, new_one, new_two, clipped,
    master, one, two, up_raw, act_raw, acts, fields, halo_out, halo_in, halo_pass, w_old, part, core_in, mine, keep,
    first, first_in, second, second_in, last_out, last_in,
    norm_out, norm_in, load_sem, send_sem, recv_sem,
):
    lat = lax.axis_index("lat")
    lon = lax.axis_index("lon")
    n_lon = n_q * 2
    core = lax.rem(lon, 2)
    q = lon // 2
    taps, rows, width = master.shape
    cols, batch, lat_rows, _ = up_raw.shape
    group_rows = batch * lat_rows
    chunks, halo_rows = halo_out.shape[1], halo_out.shape[2]
    chunk = cols // chunks
    span = chunk * group_rows
    half = width // 2
    counter = [0]
    pending, guarded = [], []

    def at(lat_id, q_id, core_id):
        return (lat_id, q_id * 2 + core_id)

    x_lat = lat + 1 - 2 * lax.rem(lat, 2)
    y_lat = lax.rem(lat + 2, 4)
    d_lat = x_lat + y_lat - lat
    partner = at(lat, q, 1 - core)
    x_peer, y_peer, d_peer = at(x_lat, q, core), at(y_lat, q, core), at(d_lat, q, core)

    def across(k):
        flipped = q
        bit = 1
        while bit < n_q:
            if k & bit:
                flipped = flipped + bit - 2 * bit * lax.rem(flipped // bit, 2)
            bit *= 2
        return flipped

    z_ids = [across(k) for k in range(n_q)]
    z_peers = [at(lat, z_ids[k], core) for k in range(1, n_q)]
    next_z, last_z = at(lat, jnp.minimum(q + 1, n_q - 1), core), at(lat, jnp.maximum(q - 1, 0), core)
    z_twins = [at(lat, z_ids[k], 1 - core) for k in range(1, n_q)]
    west = (lat, lax.rem(lon + n_lon - 1, n_lon))
    east = (lat, lax.rem(lon + 1, n_lon))
    above = (jnp.maximum(lat - 1, 0), lon)
    below = (jnp.minimum(lat + 1, n_lat - 1), lon)

    def slots(count):
        start = counter[0]
        counter[0] += count
        return start

    def remote(src, dst, target, index):
        return pltpu.make_async_remote_copy(
            src_ref=src, dst_ref=dst, send_sem=send_sem.at[index],
            recv_sem=recv_sem.at[index], device_id=target, device_id_type=MESH,
        )

    def send(src, dst, target):
        copy = remote(src, dst, target, slots(1))
        copy.start()
        pending.append(copy)
        return copy

    def send_if(condition, src, dst, target):
        copy = remote(src, dst, target, slots(1))

        @pl.when(condition)
        def _():
            copy.start()

        guarded.append((condition, copy))
        return copy

    barrier = pltpu.get_barrier_semaphore()
    greeted = [partner, x_peer, y_peer, d_peer] + z_peers + z_twins
    for device in greeted:
        pl.semaphore_signal(barrier, inc=1, device_id=device, device_id_type=MESH)

    def load(source, target, base):
        copies = [
            pltpu.make_async_copy(source.at[b], target.at[:, b], load_sem.at[base + b])
            for b in range(batch)
        ]
        for copy in copies:
            copy.start()
        return copies

    def load_whole(source, target, index):
        copy = pltpu.make_async_copy(source, target, load_sem.at[index])
        copy.start()
        return copy

    master_load = load_whole(master_hbm, master, 2 * batch)
    up_load, act_load = load(up_hbm, up_raw, 0), load(act_hbm, act_raw, batch)
    one_load = load_whole(one_hbm, one, 2 * batch + 1)
    two_load = load_whole(two_hbm, two, 2 * batch + 2)
    master_load.wait()
    for tap in range(taps):
        w_old[tap, lat, q, core] = master[tap].astype(jnp.bfloat16)

    class Gather:
        def __init__(self, buffer, cut, line_taps):
            self.buffer, self.cut = buffer, cut
            self.line_taps = line_taps
            self.line = pl.ds(0, line_taps)
            self.rest = pl.ds(line_taps, taps - line_taps)
            self.has_rest = line_taps < taps
            self.line_x = self.line_y = self.line_d = None
            self.going_up, self.going_down, self.line_core = {}, {}, []
            self.to_z, self.to_x, self.to_y, self.to_core = {}, {}, {}, []
            self.diag_x, self.diag_y = {}, {}

        def give(self, lat_id, q_id, low, high, target):
            piece = self.buffer.at[
                self.rest, lat_id, q_id, core, :, pl.ds(low, high - low)
            ]
            return send(piece, piece, target)

        def line_block(self, lat_id, q_id):
            return self.buffer.at[self.line, lat_id, q_id, core]

        def line_give(self, lat_id, target):
            piece = self.line_block(lat_id, q)
            return send(piece, piece, target)

        def line_up(self, name, lat_id, step):
            block = jnp.maximum(q - step, 0)
            piece = self.line_block(lat_id, block)
            here = q >= step
            self.going_up[name, step + 1] = send_if(
                jnp.logical_and(here, q < n_q - 1), piece, piece, next_z
            )
            if step:
                self.line_core.append((here, send_if(here, piece, piece, partner)))

        def line_down(self, name, lat_id, step):
            block = jnp.minimum(q + step, n_q - 1)
            piece = self.line_block(lat_id, block)
            here = q < n_q - step
            self.going_down[name, step + 1] = send_if(
                jnp.logical_and(here, q > 0), piece, piece, last_z
            )
            if step:
                self.line_core.append((here, send_if(here, piece, piece, partner)))

        def line_begin(self, name, lat_id):
            self.line_up(name, lat_id, 0)
            self.line_down(name, lat_id, 0)
            self.to_core.append(self.line_give(lat_id, partner))

        def line_start(self):
            if not self.line_taps:
                return
            self.line_x = self.line_give(lat, x_peer)
            self.line_begin("own", lat)

        def line_start_y(self):
            if not self.line_taps:
                return
            self.line_y = self.line_give(lat, y_peer)

        def line_cross(self):
            if not self.line_taps:
                return
            self.line_x.wait_recv()
            self.line_d = self.line_give(x_lat, y_peer)
            self.line_begin("x", x_lat)
            self.line_y.wait_recv()
            self.line_begin("y", y_lat)

        def line_far(self):
            if not self.line_taps:
                return
            self.line_d.wait_recv()
            self.line_begin("d", d_lat)

        def line_pass(self, name, lat_id, step):
            @pl.when(q >= step)
            def _():
                self.going_up[name, step].wait_recv()

            self.line_up(name, lat_id, step)

            @pl.when(q < n_q - step)
            def _():
                self.going_down[name, step].wait_recv()

            self.line_down(name, lat_id, step)

        def line_step(self, step, names=("own", "x", "y", "d")):
            if not self.line_taps or step >= n_q:
                return
            for name in names:
                self.line_pass(name, {"own": lat, "x": x_lat, "y": y_lat, "d": d_lat}[name], step)

        def core_copy(self, lat_id, k, low, high):
            if not self.has_rest:
                return
            self.to_core.append(self.give(lat_id, z_ids[k], low, high, partner))

        def start_z(self):
            if not self.has_rest:
                return
            for k in range(1, n_q):
                self.to_z[k] = self.give(lat, q, 0, width, z_peers[k - 1])

        def spread_x(self, k):
            if not self.has_rest:
                return
            self.to_x[k] = self.give(lat, z_ids[k], 0, width, x_peer)

        def spread_y(self, k):
            if not self.has_rest:
                return
            self.to_y[k] = self.give(lat, z_ids[k], 0, width, y_peer)

        def from_z(self, k):
            if not self.has_rest:
                return
            self.to_z[k].wait_recv()

        def relay_x(self, k):
            if not self.has_rest:
                return
            self.to_x[k].wait_recv()
            self.diag_y[k] = self.give(x_lat, z_ids[k], 0, self.cut, y_peer)
            self.core_copy(x_lat, k, 0, width)

        def relay_y(self, k):
            if not self.has_rest:
                return
            self.to_y[k].wait_recv()
            if self.cut < width:
                self.diag_x[k] = self.give(y_lat, z_ids[k], self.cut, width, x_peer)
            self.core_copy(y_lat, k, 0, width)

        def close(self, k):
            if not self.has_rest:
                return
            self.diag_y[k].wait_recv()
            self.core_copy(d_lat, k, 0, self.cut)
            if self.cut < width:
                self.diag_x[k].wait_recv()
                self.core_copy(d_lat, k, self.cut, width)

        def finish(self):
            for copy in self.to_core:
                copy.wait_recv()
            for condition, copy in self.line_core:
                @pl.when(condition)
                def _(copy=copy):
                    copy.wait_recv()

    def edges(field):
        to_west = send(fields.at[field, 1], fields.at[field, cols + 1], west)
        to_east = send(fields.at[field, cols], fields.at[field, 0], east)
        return to_west, to_east

    def last_row(index):
        return lax.rem(index, lat_rows) == lat_rows - 1

    def first_row(index):
        return lax.rem(index, lat_rows) == 0

    take = [
        selector((halo_rows, span), lambda m, n: n == m * lat_rows),
        selector((halo_rows, span), lambda m, n: n == m * lat_rows + lat_rows - 1),
    ]
    for copy in up_load:
        copy.wait()

    @pl.loop(0, chunks)
    def _(c):
        fields[1, pl.ds(1 + c * chunk, chunk)] = up_raw[pl.ds(c * chunk, chunk)].reshape(
            chunk, group_rows, width
        )

    pl.semaphore_wait(barrier, len(greeted))
    side_edges = {1: edges(1)}
    old = Gather(w_old, width, OLD_LINE_TAPS)
    old.line_start()
    old.start_z()
    old.core_copy(lat, 0, 0, width)
    @pl.loop(0, chunks)
    def _(c):
        block = fields[1, pl.ds(1 + c * chunk, chunk)].reshape(span, width)
        for side in range(2):
            halo_out[side, c] = jnp.dot(
                take[side], block, preferred_element_type=jnp.float32
            ).astype(jnp.bfloat16)


    near = chunks - chunks // 2
    has_above, has_below = lat > 0, lat < n_lat - 1
    inner = jnp.logical_and(has_above, has_below)
    outer = jnp.logical_not(inner)
    goes_up = lax.rem(lat, 2) == 1
    parts = (pl.ds(0, near), pl.ds(near, chunks - near))

    def halo_copy(side, part_index, target):
        piece = parts[part_index]
        return remote(
            halo_out.at[side, piece], halo_in.at[side, piece], target, slots(1)
        )

    x_side = jnp.where(goes_up, 0, 1)
    x_halo = [halo_copy(x_side, index, x_peer) for index in range(2)]
    d_halo = halo_copy(1 - x_side, 0, d_peer)
    y_halo = remote(
        halo_out.at[1 - x_side, parts[1]], halo_pass, y_peer, slots(1)
    )
    passed = remote(
        halo_pass, halo_in.at[1 - x_side, parts[1]], x_peer, slots(1)
    )

    @pl.when(inner)
    def _():
        y_halo.start()

    x_halo[0].start()
    x_halo[1].start()

    @pl.when(inner)
    def _():
        d_halo.start()

    old.line_start_y()
    old.spread_y(0)
    for copy in act_load:
        copy.wait()

    @pl.loop(0, chunks)
    def _(c):
        acts[pl.ds(c * span, span)] = act_raw[pl.ds(c * chunk, chunk)].reshape(span, width)

    part_slot = slots(taps)

    def part_copy(tap):
        return remote(
            part.at[tap, :, :, 1 - core], core_in.at[tap], partner, part_slot + tap
        )

    first_copies, second_copies, third_copies = {}, {}, {}

    order = (4, 3, 5, 1, 7, 0, 2, 6, 8)

    def reduce_tap(slot, cut):
        part_copy(slot).wait_recv()
        for k in range(n_q):
            def total(lat_id):
                return part[slot, lat_id, k, core] + core_in[slot, lat_id, k]

            mine[slot, k] = total(lat)
            first[slot, 1, k] = total(d_lat).astype(jnp.bfloat16)
            from_x, from_y = total(x_lat), total(y_lat)
            first[slot, 0, k, :, :cut] = from_y[:, :cut].astype(jnp.bfloat16)
            keep[slot, k, :, :cut] = from_x[:, :cut]
            if cut < width:
                first[slot, 0, k, :, cut:] = from_x[:, cut:].astype(jnp.bfloat16)
                keep[slot, k, :, cut:] = from_y[:, cut:]

    def weight_tap(slot):
        r, s = divmod(order[slot], 3)
        shifted = fields[r, pl.ds(2 - s, cols)].reshape(cols * group_rows, width)
        part[slot] = lax.dot_general(
            acts[...], shifted, (((0,), (0,)), ((), ())), preferred_element_type=jnp.float32,
        ).reshape(n_lat, n_q, 2, rows, width)
        part_copy(slot).start()

    def reduce_first(unit):
        low_slot, high_slot, cut = unit
        piece = pl.ds(low_slot, high_slot - low_slot)
        copies = {0: [], 1: []}
        for slot in (1, 0):
            for target, low, high in ((y_peer, 0, cut), (x_peer, cut, width)):
                if low < high:
                    lanes = pl.ds(low, high - low)
                    copies[slot].append(send(
                        first.at[piece, slot, :, :, lanes],
                        first_in.at[piece, slot, :, :, lanes], target,
                    ))
        first_copies[unit] = copies

    def reduce_second(unit):
        low_slot, high_slot, cut = unit
        for copy in first_copies[unit][1]:
            copy.wait_recv()

        @pl.loop(low_slot, high_slot)
        def _(tap):
            for k in range(n_q):
                second[tap, k] = (
                    keep[tap, k] + first_in[tap, 1, k].astype(jnp.float32)
                ).astype(jnp.bfloat16)

        piece = pl.ds(low_slot, high_slot - low_slot)
        second_copies[unit] = []
        for target, low, high in ((x_peer, 0, cut), (y_peer, cut, width)):
            if low < high:
                lanes = pl.ds(low, high - low)
                second_copies[unit].append(send(
                    second.at[piece, :, :, lanes], second_in.at[piece, :, :, lanes], target
                ))

    def reduce_third(unit):
        low_slot, high_slot, _ = unit
        for copy in first_copies[unit][0] + second_copies[unit]:
            copy.wait_recv()

        @pl.loop(low_slot, high_slot)
        def _(tap):
            for k in range(n_q):
                block = z_ids[k]
                total = (
                    mine[tap, block] + first_in[tap, 0, block].astype(jnp.float32)
                    + second_in[tap, block].astype(jnp.float32)
                )
                if k == 0:
                    mine[tap, block] = total
                else:
                    last_out[k - 1, tap] = total.astype(jnp.bfloat16)

        piece = pl.ds(low_slot, high_slot - low_slot)
        third_copies[unit] = [
            send(last_out.at[k - 1, piece], last_in.at[k - 1, piece], z_peers[k - 1])
            for k in range(1, n_q)
        ]

    def input_piece(index):
        total = None
        for tap in range(taps):
            r, s = divmod(tap, 3)
            shifted = fields[r, pl.ds(index * chunk + 2 - s, chunk)]
            product = lax.dot_general(
                shifted.reshape(span, width), w_old[tap].reshape(-1, width),
                (((1,), (1,)), ((), ())), preferred_element_type=jnp.float32,
            )
            total = product if total is None else total + product
        total = total.reshape(chunk, group_rows, width)
        for b in range(batch):
            input_grad[b, pl.ds(index * chunk, chunk)] = total[
                :, b * lat_rows : (b + 1) * lat_rows
            ].astype(jnp.bfloat16)

    def input_pieces(low, high):
        @pl.loop(low, high)
        def _(index):
            input_piece(index)

    units = [(0, 3, width), (3, 5, half), (5, 7, half), (7, 9, half)]
    weight_tap(0)
    for copy in side_edges[1]:
        copy.wait_recv()
    weight_tap(1)
    reduce_tap(0, width)
    weight_tap(2)
    reduce_tap(1, width)
    reduce_tap(2, width)
    reduce_first(units[0])
    @pl.when(outer)
    def _():
        y_halo.wait_recv()
        passed.start()

    old.line_cross()
    old.line_step(1, ("own",))
    for copy in x_halo:
        copy.wait_recv()

    @pl.when(inner)
    def _():
        d_halo.wait_recv()
        passed.wait_recv()

    @pl.when(jnp.logical_not(has_below))
    def _():
        halo_in[0] = jnp.zeros(halo_in.shape[1:], halo_in.dtype)

    @pl.when(jnp.logical_not(has_above))
    def _():
        halo_in[1] = jnp.zeros(halo_in.shape[1:], halo_in.dtype)

    shift = [
        selector((span, span), lambda m, n: jnp.logical_and(n == m + 1, jnp.logical_not(last_row(m)))),
        selector((span, span), lambda m, n: jnp.logical_and(n == m - 1, jnp.logical_not(first_row(m)))),
    ]
    place = [
        selector((span, halo_rows), lambda m, n: jnp.logical_and(n == m // lat_rows, last_row(m))),
        selector((span, halo_rows), lambda m, n: jnp.logical_and(n == m // lat_rows, first_row(m))),
    ]

    @pl.loop(0, chunks)
    def _(c):
        block = fields[1, pl.ds(1 + c * chunk, chunk)].reshape(span, width)
        for side in range(2):
            moved = jnp.dot(shift[side], block, preferred_element_type=jnp.float32)
            moved = moved + jnp.dot(
                place[side], halo_in[side, c], preferred_element_type=jnp.float32
            )
            fields[2 * side, pl.ds(1 + c * chunk, chunk)] = moved.astype(jnp.bfloat16).reshape(
                chunk, group_rows, width
            )

    side_edges[0], side_edges[2] = edges(0), edges(2)
    old.line_step(1, ("x", "y"))
    old.line_step(2, ("own",))
    weight_tap(3)
    weight_tap(4)
    reduce_second(units[0])
    reduce_tap(3, half)
    reduce_tap(4, half)
    reduce_first(units[1])
    old.line_far()
    old.line_step(2, ("x", "y"))
    old.line_step(3, ("own",))
    for copy in side_edges[0] + side_edges[2]:
        copy.wait_recv()
    weight_tap(5)
    weight_tap(6)
    reduce_tap(5, half)
    reduce_tap(6, half)
    reduce_first(units[2])
    old.line_step(1, ("d",))
    old.line_step(3, ("x", "y"))
    weight_tap(7)
    weight_tap(8)
    reduce_tap(7, half)
    reduce_tap(8, half)
    reduce_first(units[3])
    old.line_step(2, ("d",))
    reduce_second(units[1])
    reduce_third(units[0])
    reduce_second(units[2])
    reduce_third(units[1])
    reduce_second(units[3])
    for k in range(1, n_q):
        old.from_z(k)
        old.spread_y(k)
        old.core_copy(lat, k, 0, width)
    for k in range(n_q):
        old.spread_x(k)
    reduce_third(units[2])
    reduce_third(units[3])
    for k in range(n_q):
        old.relay_y(k)
        old.relay_x(k)
    old.line_step(3, ("d",))
    for step in range(4, n_q):
        old.line_step(step)
    for unit in units:
        for copy in third_copies[unit]:
            copy.wait_recv()
    square = jnp.zeros((rows, width), jnp.float32)
    for index, tap in enumerate(order):
        grad = mine[index, q]
        for k in range(n_q - 1):
            grad = grad + last_in[k, index].astype(jnp.float32)
        clipped[tap] = grad
        square = square + grad * grad
    square = jnp.sum(square)
    slot = 0
    fill = [chunks // 2, chunks // 6]
    done = 0
    for stage, peers in enumerate(([partner] + z_peers + z_twins, [x_peer, y_peer, d_peer])):
        norm_out[stage] = jnp.full(norm_out.shape[1:], square, jnp.float32)
        copies = []
        for index, target in enumerate(peers):
            copies.append(send(norm_out.at[stage], norm_in.at[slot + index], target))
        if stage == 0:
            for k in range(n_q):
                old.close(k)
            old.finish()
        input_pieces(done, done + fill[stage])
        done += fill[stage]
        tile = norm_out[stage]
        for index, copy in enumerate(copies):
            copy.wait_recv()
            tile = tile + norm_in[slot + index]
        slot += len(peers)
        square = jnp.max(tile)
    one_load.wait()
    two_load.wait()
    square = jnp.full((1, 1), square, jnp.float32)
    clip_factor = jnp.minimum(1.0, max_norm / (jnp.sqrt(square) + norm_eps))

    @pl.loop(0, taps)
    def _(tap):
        scaled = clip_factor * clipped[tap]
        clipped[tap] = scaled
        moment = beta_one * one[tap] + (1.0 - beta_one) * scaled
        spread = beta_two * two[tap] + (1.0 - beta_two) * scaled * scaled
        new_one[tap] = moment
        new_two[tap] = spread
        first_hat = moment / (1.0 - beta_one**step_count)
        second_hat = spread / (1.0 - beta_two**step_count)
        updated = master[tap] - learn_rate * (
            first_hat / (jnp.sqrt(second_hat) + adam_eps) + decay_rate * master[tap]
        )
        new_master[tap] = updated
        w_new[tap, lat, q, core] = updated.astype(jnp.bfloat16)

    new = Gather(w_new, half, NEW_LINE_TAPS)
    new.line_start()
    new.line_start_y()
    new.start_z()
    new.spread_x(0)
    new.spread_y(0)
    new.core_copy(lat, 0, 0, width)
    input_pieces(done, chunks)
    new.line_cross()
    for k in range(1, n_q):
        new.from_z(k)
        new.spread_x(k)
        new.spread_y(k)
        new.core_copy(lat, k, 0, width)
        new.relay_x(k - 1)
        new.relay_y(k - 1)
        if k == 1:
            new.line_far()
        new.line_step(k)
    new.relay_x(n_q - 1)
    new.relay_y(n_q - 1)
    for k in range(n_q):
        new.close(k)
    new.finish()

    for copy in x_halo:
        copy.wait_send()

    @pl.when(inner)
    def _():
        y_halo.wait_send()
        d_halo.wait_send()

    @pl.when(outer)
    def _():
        passed.wait_send()

    @pl.loop(0, taps)
    def _(tap):
        part_copy(tap).wait_send()

    for copy in pending:
        copy.wait_send()
    for condition, copy in guarded:
        @pl.when(condition)
        def _(copy=copy):
            copy.wait_send()


def land(*refs):
    count = len(refs) // 2
    sources, targets, sem = refs[:count], refs[count : 2 * count], refs[-1]
    copies = [
        pltpu.make_async_copy(source, target, sem.at[index])
        for index, (source, target) in enumerate(zip(sources, targets))
    ]
    for copy in copies:
        copy.start()
    for copy in copies:
        copy.wait()


def landed(arrays):
    anywhere = pl.BlockSpec(memory_space=pl.ANY)
    return pl.pallas_call(
        land,
        out_shape=tuple(jax.ShapeDtypeStruct(a.shape, a.dtype) for a in arrays),
        in_specs=[anywhere] * len(arrays),
        out_specs=(anywhere,) * len(arrays),
        scratch_shapes=[pltpu.SemaphoreType.DMA((len(arrays),))],
        compiler_params=pltpu.CompilerParams(vmem_limit_bytes=1024 * 1024),
        name="land",
    )(*arrays)


def fused_step(up, act, master, one, two):
    n_lat, n_q = lax.axis_size("lat"), lax.axis_size("lon") // 2
    taps, rows, width = master.shape
    batch, cols, lat_rows, _ = up.shape
    group_rows = batch * lat_rows
    chunk = max(c for c in range(1, 17) if cols % c == 0)
    chunks = cols // chunk
    halo_rows = -(-chunk * batch // ROW_TILE) * ROW_TILE
    max_norm = math.sqrt(float(n_lat * n_q * 2 * taps * rows * width))
    bf16, f32 = jnp.bfloat16, jnp.float32
    shard = pltpu.VMEM(master.shape, f32)
    whole = (taps, n_lat, n_q, 2, rows, width)
    lat_block = (taps, n_q, rows, width)
    vmem, hbm = (pl.BlockSpec(memory_space=m) for m in (pltpu.VMEM, pltpu.HBM))
    peers = 2 * n_q + n_lat - 2
    copies = 192 + 32 * (n_q + n_lat)
    return pl.pallas_call(
        functools.partial(whole_step, n_lat, n_q, max_norm),
        out_shape=(
            pltpu.VMEM(up.shape, bf16), pltpu.VMEM(whole, bf16), shard, shard, shard, shard,
        ),
        in_specs=[hbm] * 5,
        out_specs=(vmem,) * 6,
        scratch_shapes=[
            pltpu.VMEM(master.shape, f32),
            pltpu.VMEM(master.shape, f32),
            pltpu.VMEM(master.shape, f32),
            pltpu.VMEM((cols, batch, lat_rows, width), bf16),
            pltpu.VMEM((cols, batch, lat_rows, width), bf16),
            pltpu.VMEM((cols * group_rows, width), bf16),
            pltpu.VMEM((3, cols + 2, group_rows, width), bf16),
            pltpu.VMEM((2, chunks, halo_rows, width), bf16),
            pltpu.VMEM((2, chunks, halo_rows, width), bf16),
            pltpu.VMEM((chunks // 2, halo_rows, width), bf16),
            pltpu.VMEM(whole, bf16),
            pltpu.VMEM(whole, f32),
            pltpu.VMEM((taps, n_lat, n_q, rows, width), f32),
            pltpu.VMEM(lat_block, f32),
            pltpu.VMEM(lat_block, f32),
            pltpu.VMEM((taps, 2, n_q, rows, width), bf16),
            pltpu.VMEM((taps, 2, n_q, rows, width), bf16),
            pltpu.VMEM(lat_block, bf16),
            pltpu.VMEM(lat_block, bf16),
            pltpu.VMEM((n_q - 1, taps, rows, width), bf16),
            pltpu.VMEM((n_q - 1, taps, rows, width), bf16),
            pltpu.VMEM((3, 8, LANE_TILE), f32),
            pltpu.VMEM((peers, 8, LANE_TILE), f32),
            pltpu.SemaphoreType.DMA((2 * batch + 3,)),
            pltpu.SemaphoreType.DMA((copies,)),
            pltpu.SemaphoreType.DMA((copies,)),
        ],
        compiler_params=pltpu.CompilerParams(
            collective_id=2, has_side_effects=True, vmem_limit_bytes=48 * 1024 * 1024
        ),
        name="whole_step",
    )(up, act, master, one, two)


def takes_fused(activations, master):
    n_lat, n_q = lax.axis_size("lat"), lax.axis_size("lon") // 2
    batch, lat_rows, cols, _ = activations.shape
    return (
        n_lat == 4 and n_q & (n_q - 1) == 0 and n_q > 1 and master.shape[0] % ROW_TILE == 0
        and (batch * lat_rows) % ROW_TILE == 0 and cols % 2 == 0
        and master.shape[2] % (2 * LANE_TILE) == 0 and master.shape[1] == 9
    )


def per_device(activations, upstream, master, moment_one, moment_two):
    if not takes_fused(activations, master):
        return per_device_general(activations, upstream, master, moment_one, moment_two)

    def by_col(field):
        return jnp.transpose(field, (0, 2, 1, 3))

    def by_tap(array):
        return jnp.transpose(array, (1, 0, 2))

    input_grad, gathered, new_master, new_one, new_two, clipped = landed(fused_step(
        by_col(upstream), by_col(activations), by_tap(master), by_tap(moment_one),
        by_tap(moment_two),
    ))
    new_weights = by_tap(gathered.reshape(gathered.shape[0], -1, gathered.shape[-1]))
    return (
        by_col(input_grad), new_weights, by_tap(new_master), by_tap(new_one), by_tap(new_two),
        by_tap(clipped),
    )


def per_device_general(activations, upstream, master, moment_one, moment_two):
    lat_rows = activations.shape[1]
    lon_cols = activations.shape[2]
    grad_flat = upstream.reshape(-1, upstream.shape[3])
    old_weights = master[:, ::-1].astype(jnp.bfloat16)
    old_full = lax.all_gather(old_weights, ("lat", "lon"), axis=0, tiled=True)
    act_wide, grad_wide = widened((activations, upstream))
    term_maker = input_taps(act_wide, grad_flat, lat_rows, lon_cols)
    partial = term_maker(jnp.int32(0), activations.shape[3])

    def by_tap(array):
        return jnp.transpose(array, (1, 0, 2))

    gathered, new_master, new_one, new_two, clipped = fused_update(
        by_tap(partial), by_tap(master), by_tap(moment_one), by_tap(moment_two)
    )
    new_weights = jnp.transpose(gathered, (2, 1, 0, 4, 3, 5)).reshape(
        activations.shape[3], gathered.shape[3], gathered.shape[5]
    )
    old_full, new_one = lax.optimization_barrier((old_full, new_one))
    input_grad = lax.conv_general_dilated(
        grad_wide,
        old_full.reshape(old_full.shape[0], 3, 3, old_full.shape[2]),
        (1, 1),
        "VALID",
        dimension_numbers=("NHWC", "OHWI", "NHWC"),
        preferred_element_type=jnp.float32,
    ).astype(jnp.bfloat16)
    return (
        input_grad, new_weights, by_tap(new_master), by_tap(new_one), by_tap(new_two),
        by_tap(clipped),
    )


def solution(mesh):
    in_specs = (
        P(None, "lat", "lon", None),
        P(None, "lat", "lon", None),
        P(("lat", "lon"), None, None),
        P(("lat", "lon"), None, None),
        P(("lat", "lon"), None, None),
    )
    out_specs = (
        P(None, "lat", "lon", None),
        P(),
        P(("lat", "lon"), None, None),
        P(("lat", "lon"), None, None),
        P(("lat", "lon"), None, None),
        P(("lat", "lon"), None, None),
    )
    return jax.shard_map(
        per_device, mesh=mesh, in_specs=in_specs, out_specs=out_specs, check_vma=False
    )
```

```python
import functools
import math

import jax
import jax.numpy as jnp
from jax import lax
from jax.experimental import pallas as pl
from jax.experimental.pallas import tpu as pltpu
from jax.sharding import PartitionSpec as P

MESH = pl.DeviceIdType.MESH

CIN = 512
COUT = 512
TAPS = 9


learn_rate = 0.01
beta_one = 0.9
beta_two = 0.999
adam_eps = 1e-08
decay_rate = 0.1
step_count = 10.0
norm_eps = 1e-06


def halo_kernel(n_lat, n_lon, *refs):
    sources, landings, (send_sem, recv_sem) = refs[:8], refs[8:16], refs[16:]
    lat, lon = lax.axis_index("lat"), lax.axis_index("lon")
    steps = ((-1, 0), (1, 0), (0, -1), (0, 1), (-1, -1), (-1, 1), (1, -1), (1, 1))
    targets = [
        (lax.rem(lat + dy + n_lat, n_lat), lax.rem(lon + dx + n_lon, n_lon)) for dy, dx in steps
    ]
    barrier = pltpu.get_barrier_semaphore()
    for target in targets:
        pl.semaphore_signal(barrier, inc=1, device_id=target, device_id_type=MESH)
    pl.semaphore_wait(barrier, len(targets))
    copies = []
    for index, target in enumerate(targets):
        copy = pltpu.make_async_remote_copy(
            src_ref=sources[index], dst_ref=landings[index], send_sem=send_sem.at[index],
            recv_sem=recv_sem.at[index], device_id=target, device_id_type=MESH,
        )
        copy.start()
        copies.append(copy)
    for copy in copies:
        copy.wait()


def widened(fields):
    both = jnp.stack(fields)
    top, bottom = both[:, :, 0], both[:, :, -1]
    pieces = (
        top, bottom, both[:, :, :, 0], both[:, :, :, -1],
        top[:, :, 0], top[:, :, -1], bottom[:, :, 0], bottom[:, :, -1],
    )
    landed = pl.pallas_call(
        functools.partial(halo_kernel, lax.axis_size("lat"), lax.axis_size("lon")),
        out_shape=tuple(jax.ShapeDtypeStruct(p.shape, p.dtype) for p in pieces),
        in_specs=[pl.BlockSpec(memory_space=pltpu.VMEM)] * 8,
        out_specs=(pl.BlockSpec(memory_space=pltpu.VMEM),) * 8,
        scratch_shapes=[pltpu.SemaphoreType.DMA((8,)), pltpu.SemaphoreType.DMA((8,))],
        compiler_params=pltpu.CompilerParams(
            collective_id=1, has_side_effects=True, vmem_limit_bytes=24 * 1024 * 1024
        ),
        name="halo",
    )(*pieces)
    below, above, east, west, below_east, below_west, above_east, above_west = landed

    def row(start, middle, end):
        return jnp.concatenate([start[:, None, None], middle[:, None], end[:, None, None]], axis=2)

    wide = []
    for index, field in enumerate(fields):
        middle = jnp.concatenate(
            [west[index][:, :, None], field, east[index][:, :, None]], axis=2
        )
        first = row(above_west[index], above[index], above_east[index])
        last = row(below_west[index], below[index], below_east[index])
        wide.append(mask_poles(jnp.concatenate([first, middle, last], axis=1)))
    return wide


def mask_poles(wide_field):
    lat_index = lax.axis_index("lat")
    lat_count = lax.axis_size("lat")
    total_rows = wide_field.shape[1]
    row_ids = lax.broadcasted_iota(jnp.int32, (1, total_rows, 1, 1), 1)
    upper = jnp.logical_and(row_ids == 0, lat_index == 0)
    lower = jnp.logical_and(row_ids == total_rows - 1, lat_index == lat_count - 1)
    return jnp.where(jnp.logical_or(upper, lower), jnp.zeros((), wide_field.dtype), wide_field)


def input_taps(act_wide, grad_flat, lat_rows, lon_cols):

    def input_compute(first_row, row_count):
        tap_parts = []
        for tap_index in range(9):
            row_off, col_off = divmod(tap_index, 3)
            tap_slab = act_wide[
                :, row_off : row_off + lat_rows, col_off : col_off + lon_cols, :
            ].reshape(-1, row_count)
            tap_parts.append(
                lax.dot_general(
                    tap_slab,
                    grad_flat,
                    (((0,), (0,)), ((), ())),
                    preferred_element_type=jnp.float32,
                )
            )
        return jnp.stack(tap_parts, axis=1)

    return input_compute


def reduce_update_gather(
    n_lat, n_q, max_norm, part, master, one, two,
    gathered, new_master, new_one, new_two, clipped,
    core_in, sums, right_in, left_in, lat_out, lat_in, norm_out, norm_in,
    send_sem, recv_sem,
):
    lat = lax.axis_index("lat")
    lon = lax.axis_index("lon")
    core = lax.rem(lon, 2)
    q = lon // 2
    hops = n_q // 2
    half = n_lat // 2
    counter = [0]
    pending = []

    def at(lat_id, q_id, core_id):
        return (lat_id, q_id * 2 + core_id)

    partner = at(lat, q, 1 - core)
    right_q = lax.rem(q + 1, n_q)
    left_q = lax.rem(q + n_q - 1, n_q)
    right, left = at(lat, right_q, core), at(lat, left_q, core)
    q_peers = [at(lat, lax.rem(q + d, n_q), core) for d in range(1, n_q)]
    lat_peers = [at(lax.rem(lat + d, n_lat), q, core) for d in range(1, n_lat)]

    def send(src, dst, target):
        index = counter[0]
        counter[0] += 1
        copy = pltpu.make_async_remote_copy(
            src_ref=src, dst_ref=dst, send_sem=send_sem.at[index],
            recv_sem=recv_sem.at[index], device_id=target, device_id_type=MESH,
        )
        copy.start()
        pending.append(copy)
        return copy

    def wrap(index, size):
        return lax.rem(index + size, size)

    barrier = pltpu.get_barrier_semaphore()
    greeted = [partner] + q_peers + lat_peers
    for device in greeted:
        pl.semaphore_signal(barrier, inc=1, device_id=device, device_id_type=MESH)
    pl.semaphore_wait(barrier, len(greeted))

    order = []
    for step in range(hops):
        for block in (hops - step, -hops + step):
            if block % n_q not in order:
                order.append(block % n_q)
    order.append(0)
    core_copies = []
    for offset in order:
        block = lax.rem(q + offset, n_q)
        core_copies.append(
            send(part.at[:, :, block, 1 - core], core_in.at[:, :, block], partner)
        )
    arrived = {}

    def core_sum(offset):
        if offset in arrived:
            return
        arrived[offset] = True
        core_copies[order.index(offset)].wait_recv()
        block = lax.rem(q + offset, n_q)

        @pl.loop(0, n_lat)
        def _(row):
            sums[block, row] = (
                part[:, row, block, core] + core_in[:, row, block]
            ).astype(jnp.bfloat16)

    def add_into(block, low, high, source):
        @pl.loop(low, high)
        def _(row):
            sums[block, row] = (
                sums[block, row].astype(jnp.float32) + source[row].astype(jnp.float32)
            ).astype(jnp.bfloat16)

    ring = []
    for step in range(hops):
        right_off = (hops - step) % n_q
        left_off = (step - hops) % n_q
        core_sum(right_off)
        core_sum(left_off)
        right_block = lax.rem(q + right_off, n_q)
        left_block = lax.rem(q + left_off, n_q)
        if step == 0:
            ring.append((
                send(sums.at[right_block, pl.ds(0, half)], right_in.at[0, pl.ds(0, half)], right),
                send(sums.at[left_block, pl.ds(half, n_lat - half)],
                     left_in.at[0, pl.ds(half, n_lat - half)], left),
            ))
        else:
            from_left, from_right = ring[-1]
            bounds = (0, half, half, n_lat) if step == 1 else (0, n_lat, 0, n_lat)
            from_left.wait_recv()
            add_into(right_block, bounds[0], bounds[1], right_in.at[step - 1])
            going_right = send(sums.at[right_block], right_in.at[step], right)
            from_right.wait_recv()
            add_into(left_block, bounds[2], bounds[3], left_in.at[step - 1])
            ring.append((going_right, send(sums.at[left_block], left_in.at[step], left)))
    core_sum(0)
    for copy in ring[-1]:
        copy.wait_recv()

    def q_total(row):
        total = part[:, row, q, core] + core_in[:, row, q]
        if hops > 1:
            return (
                total + right_in[hops - 1, row].astype(jnp.float32)
                + left_in[hops - 1, row].astype(jnp.float32)
            )
        return total + jnp.where(
            row < half, right_in[0, row].astype(jnp.float32), left_in[0, row].astype(jnp.float32)
        )

    lat_copies = []
    for step in range(1, n_lat):
        target = lax.rem(lat + step, n_lat)
        lat_out[step - 1] = q_total(target).astype(jnp.bfloat16)
        lat_copies.append(send(lat_out.at[step - 1], lat_in.at[step - 1], lat_peers[step - 1]))
    grad = q_total(lat)
    for step, copy in enumerate(lat_copies):
        copy.wait_recv()
        grad = grad + lat_in[step].astype(jnp.float32)
    clipped[...] = grad

    square = jnp.sum(grad * grad)
    slot = 0
    for stage, peers in enumerate(([partner], q_peers, lat_peers)):
        norm_out[stage] = jnp.full(norm_out.shape[1:], square, jnp.float32)
        copies = []
        for target in peers:
            copies.append(send(norm_out.at[stage], norm_in.at[slot], target))
            slot += 1
        tile = norm_out[stage]
        for index, copy in enumerate(copies):
            copy.wait_recv()
            tile = tile + norm_in[slot - len(peers) + index]
        square = jnp.max(tile)
    square = jnp.full((1, 1), square, jnp.float32)
    clip_factor = jnp.minimum(1.0, max_norm / (jnp.sqrt(square) + norm_eps))

    @pl.loop(0, clipped.shape[0])
    def _(tap):
        scaled = clip_factor * clipped[tap]
        clipped[tap] = scaled
        first = beta_one * one[tap] + (1.0 - beta_one) * scaled
        second = beta_two * two[tap] + (1.0 - beta_two) * scaled * scaled
        new_one[tap] = first
        new_two[tap] = second
        first_hat = first / (1.0 - beta_one**step_count)
        second_hat = second / (1.0 - beta_two**step_count)
        updated = master[tap] - learn_rate * (
            first_hat / (jnp.sqrt(second_hat) + adam_eps) + decay_rate * master[tap]
        )
        new_master[tap] = updated
        gathered[core, q, lat, tap] = updated.astype(jnp.bfloat16)

    copies = [
        send(gathered.at[core, q, lat], gathered.at[core, q, lat], peer) for peer in lat_peers
    ]
    for copy in copies:
        copy.wait_recv()
    core_in_copies = []

    def to_partner(block, low, count):
        piece = gathered.at[core, block, pl.ds(low, count)]
        core_in_copies.append(send(piece, piece, partner))

    from_left = from_right = None
    for step in range(hops):
        last = step == hops - 1
        right_block = wrap(q - step, n_q)
        left_block = lax.rem(q + step, n_q)
        if from_left is not None:
            from_left.wait_recv()
        piece = gathered.at[core, right_block, pl.ds(0, half if last else n_lat)]
        going_right = send(piece, piece, right)
        if from_right is not None:
            from_right.wait_recv()
        low = half if last else 0
        piece = gathered.at[core, left_block, pl.ds(low, n_lat - low)]
        going_left = send(piece, piece, left)
        to_partner(right_block, 0, n_lat)
        if step > 0:
            to_partner(left_block, 0, n_lat)
        from_left, from_right = going_right, going_left
    far = lax.rem(q + hops, n_q)
    from_left.wait_recv()
    to_partner(far, 0, half)
    from_right.wait_recv()
    to_partner(far, half, n_lat - half)
    for copy in core_in_copies:
        copy.wait_recv()
    for copy in pending:
        copy.wait_send()


def fused_update(partial, master, one, two):
    n_lat, n_q = lax.axis_size("lat"), lax.axis_size("lon") // 2
    taps, rows, width = master.shape
    part = partial.reshape(taps, n_lat, n_q, 2, rows, width)
    max_norm = math.sqrt(float(partial.size))
    shard = jax.ShapeDtypeStruct(master.shape, jnp.float32)
    hops = n_q // 2
    half_type = jnp.bfloat16
    block = (n_lat, taps, rows, width)
    peers = n_q + n_lat - 1
    vmem = pl.BlockSpec(memory_space=pltpu.VMEM)
    copies = 64 + 8 * (n_q + n_lat)
    return pl.pallas_call(
        functools.partial(reduce_update_gather, n_lat, n_q, max_norm),
        out_shape=(
            jax.ShapeDtypeStruct((2, n_q) + block, half_type), shard, shard, shard, shard,
        ),
        in_specs=[vmem] * 4,
        out_specs=(vmem,) * 5,
        scratch_shapes=[
            pltpu.VMEM((taps, n_lat, n_q, rows, width), jnp.float32),
            pltpu.VMEM((n_q,) + block, half_type),
            pltpu.VMEM((hops,) + block, half_type),
            pltpu.VMEM((hops,) + block, half_type),
            pltpu.VMEM((n_lat - 1, taps, rows, width), half_type),
            pltpu.VMEM((n_lat - 1, taps, rows, width), half_type),
            pltpu.VMEM((3, 8, 128), jnp.float32),
            pltpu.VMEM((peers, 8, 128), jnp.float32),
            pltpu.SemaphoreType.DMA((copies,)),
            pltpu.SemaphoreType.DMA((copies,)),
        ],
        compiler_params=pltpu.CompilerParams(
            collective_id=0, has_side_effects=True, vmem_limit_bytes=60 * 1024 * 1024
        ),
        name="reduce_update_gather",
    )(part, master, one, two)


LANE_TILE = 128
ROW_TILE = 16
OLD_LINE_TAPS = 6
NEW_LINE_TAPS = 2


def selector(shape, rows_of):
    rows = lax.broadcasted_iota(jnp.int32, shape, 0)
    cols = lax.broadcasted_iota(jnp.int32, shape, 1)
    return jnp.where(rows_of(rows, cols), 1.0, 0.0).astype(jnp.bfloat16)


def whole_step(
    n_lat, n_q, max_norm,
    up_hbm, act_hbm, master_hbm, one_hbm, two_hbm,
    input_grad, w_new, new_master, new_one, new_two, clipped,
    master, one, two, up_raw, act_raw, acts, fields, halo_out, halo_in, halo_pass, w_old, part, core_in, mine, keep,
    first, first_in, second, second_in, last_out, last_in,
    norm_out, norm_in, load_sem, send_sem, recv_sem,
):
    lat = lax.axis_index("lat")
    lon = lax.axis_index("lon")
    n_lon = n_q * 2
    core = lax.rem(lon, 2)
    q = lon // 2
    taps, rows, width = master.shape
    cols, batch, lat_rows, _ = up_raw.shape
    group_rows = batch * lat_rows
    chunks, halo_rows = halo_out.shape[1], halo_out.shape[2]
    chunk = cols // chunks
    span = chunk * group_rows
    half = width // 2

    def at(lat_id, q_id, core_id):
        return (lat_id, q_id * 2 + core_id)

    x_lat = lat + 1 - 2 * lax.rem(lat, 2)
    y_lat = lax.rem(lat + 2, 4)
    d_lat = x_lat + y_lat - lat
    partner = at(lat, q, 1 - core)
    x_peer, y_peer, d_peer = at(x_lat, q, core), at(y_lat, q, core), at(d_lat, q, core)

    def across(k):
        flipped = q
        bit = 1
        while bit < n_q:
            if k & bit:
                flipped = flipped + bit - 2 * bit * lax.rem(flipped // bit, 2)
            bit *= 2
        return flipped

    z_ids = [across(k) for k in range(n_q)]
    z_peers = [at(lat, z_ids[k], core) for k in range(1, n_q)]
    next_z, last_z = at(lat, jnp.minimum(q + 1, n_q - 1), core), at(lat, jnp.maximum(q - 1, 0), core)
    z_twins = [at(lat, z_ids[k], 1 - core) for k in range(1, n_q)]
    west = (lat, lax.rem(lon + n_lon - 1, n_lon))
    east = (lat, lax.rem(lon + 1, n_lon))
    above = (jnp.maximum(lat - 1, 0), lon)
    below = (jnp.minimum(lat + 1, n_lat - 1), lon)

    used = [0, 0]
    closing = []

    def remote(src, dst, target, sent, landed_at):
        return pltpu.make_async_remote_copy(
            src_ref=src, dst_ref=dst, send_sem=send_sem.at[sent],
            recv_sem=recv_sem.at[landed_at], device_id=target, device_id_type=MESH,
        )

    def landing(count=1):
        used[1] += count
        return used[1] - count

    def outgoing(view, condition=None):
        used[0] += 1
        closing.append((condition, remote(view, view, partner, used[0] - 1, 0)))
        return used[0] - 1

    def arrived(view, landed_at):
        remote(view, view, partner, 0, landed_at).wait_recv()

    def send(src, dst, target, sent, landed_at):
        remote(src, dst, target, sent, landed_at).start()

    barrier = pltpu.get_barrier_semaphore()
    greeted = [partner, x_peer, y_peer, d_peer] + z_peers + z_twins
    for device in greeted:
        pl.semaphore_signal(barrier, inc=1, device_id=device, device_id_type=MESH)

    def load(source, target, base):
        copies = [
            pltpu.make_async_copy(source.at[b], target.at[:, b], load_sem.at[base + b])
            for b in range(batch)
        ]
        for copy in copies:
            copy.start()
        return copies

    def load_whole(source, target, index):
        copy = pltpu.make_async_copy(source, target, load_sem.at[index])
        copy.start()
        return copy

    master_load = load_whole(master_hbm, master, 2 * batch)
    up_load, act_load = load(up_hbm, up_raw, 0), load(act_hbm, act_raw, batch)
    one_load = load_whole(one_hbm, one, 2 * batch + 1)
    two_load = load_whole(two_hbm, two, 2 * batch + 2)
    master_load.wait()
    for tap in range(taps):
        w_old[tap, lat, q, core] = master[tap].astype(jnp.bfloat16)

    class Gather:
        def __init__(self, buffer, cut, line_taps):
            self.buffer, self.cut, self.line_taps = buffer, cut, line_taps
            self.line = pl.ds(0, line_taps)
            self.rest = pl.ds(line_taps, taps - line_taps)
            self.has_rest = line_taps < taps
            self.core_sent = outgoing(buffer.at[:, :, :, core])
            self.core_landed = landing()
            self.sent, self.landed = {}, {}
            if self.has_rest:
                for name, view in (
                    ("z", buffer.at[self.rest, lat, pl.ds(0, n_q - 1), core]),
                    ("x", buffer.at[self.rest, lat, :, core]),
                    ("y", buffer.at[self.rest, lat, :, core]),
                    ("low", buffer.at[self.rest, x_lat, :, core, :, pl.ds(0, cut)]),
                ):
                    self.sent[name], self.landed[name] = outgoing(view), landing(n_q)
                if cut < width:
                    lanes = pl.ds(cut, width - cut)
                    self.sent["high"] = outgoing(
                        buffer.at[self.rest, y_lat, :, core, :, lanes]
                    )
                    self.landed["high"] = landing(n_q)
            if line_taps:
                for name in ("line_x", "line_y", "line_d"):
                    self.sent[name] = outgoing(self.line_block(lat, q))
                    self.landed[name] = landing()
                for step in range(n_q - 1):
                    plane = buffer.at[self.line, :, q, core]
                    self.sent["up", step] = outgoing(
                        plane, jnp.logical_and(q >= step, q < n_q - 1)
                    )
                    self.sent["down", step] = outgoing(
                        plane, jnp.logical_and(q < n_q - step, q > 0)
                    )
                    for name in ("own", "xy", "d"):
                        self.landed["up", name, step + 1] = landing()
                        self.landed["down", name, step + 1] = landing()

        def block(self, lat_id, q_id, low, high):
            return self.buffer.at[
                self.rest, lat_id, q_id, core, :, pl.ds(low, high - low)
            ]

        def give(self, name, k, lat_id, q_id, low, high, target):
            piece = self.block(lat_id, q_id, low, high)
            send(piece, piece, target, self.sent[name], self.landed[name] + k)

        def take(self, name, k, low, high):
            arrived(self.block(lat, q, low, high), self.landed[name] + k)

        def core_copy(self, lat_id, k, low, high):
            if self.has_rest:
                piece = self.block(lat_id, z_ids[k], low, high)
                send(piece, piece, partner, self.core_sent, self.core_landed)

        def line_block(self, lat_id, q_id):
            return self.buffer.at[self.line, lat_id, q_id, core]

        def line_give(self, name, lat_id, target):
            piece = self.line_block(lat_id, q)
            send(piece, piece, target, self.sent[name], self.landed[name])

        def line_take(self, name):
            arrived(self.line_block(lat, q), self.landed[name])

        def line_core(self, lat_id, q_id):
            piece = self.line_block(lat_id, q_id)
            send(piece, piece, partner, self.core_sent, self.core_landed)

        def line_pass(self, name, lat_ids, step):
            for way, here, ahead, block, target in (
                ("up", q >= step, q < n_q - 1, jnp.maximum(q - step, 0), next_z),
                ("down", q < n_q - step, q > 0, jnp.minimum(q + step, n_q - 1), last_z),
            ):
                if step:
                    @pl.when(here)
                    def _():
                        view = self.buffer.at[self.line, pl.ds(0, len(lat_ids)), q, core]
                        arrived(view, self.landed[way, name, step])
                        for lat_id in lat_ids:
                            self.line_core(lat_id, block)

                if step < n_q - 1:
                    @pl.when(jnp.logical_and(here, ahead))
                    def _():
                        for lat_id in lat_ids:
                            piece = self.line_block(lat_id, block)
                            send(
                                piece, piece, target, self.sent[way, step],
                                self.landed[way, name, step + 1],
                            )

        def line_step(self, step, names=("own", "xy", "d")):
            if not self.line_taps or step >= n_q:
                return
            for name in names:
                lat_ids = {"own": (lat,), "xy": (x_lat, y_lat), "d": (d_lat,)}[name]
                self.line_pass(name, lat_ids, step)

        def line_start(self):
            if self.line_taps:
                self.line_give("line_x", lat, x_peer)
                self.line_step(0, ("own",))
                self.line_core(lat, q)

        def line_start_y(self):
            if self.line_taps:
                self.line_give("line_y", lat, y_peer)

        def line_cross(self):
            if self.line_taps:
                self.line_take("line_x")
                self.line_give("line_d", x_lat, y_peer)
                self.line_core(x_lat, q)
                self.line_take("line_y")
                self.line_core(y_lat, q)
                self.line_step(0, ("xy",))

        def line_far(self):
            if self.line_taps:
                self.line_take("line_d")
                self.line_core(d_lat, q)
                self.line_step(0, ("d",))

        def start_z(self):
            if self.has_rest:
                for k in range(1, n_q):
                    self.give("z", k, lat, q, 0, width, z_peers[k - 1])

        def spread_x(self, k):
            if self.has_rest:
                self.give("x", k, lat, z_ids[k], 0, width, x_peer)

        def spread_y(self, k):
            if self.has_rest:
                self.give("y", k, lat, z_ids[k], 0, width, y_peer)

        def from_z(self, k):
            if self.has_rest:
                self.take("z", k, 0, width)

        def relay_x(self, k):
            if self.has_rest:
                self.take("x", k, 0, width)
                self.give("low", k, x_lat, z_ids[k], 0, self.cut, y_peer)
                self.core_copy(x_lat, k, 0, width)

        def relay_y(self, k):
            if self.has_rest:
                self.take("y", k, 0, width)
                if self.cut < width:
                    self.give("high", k, y_lat, z_ids[k], self.cut, width, x_peer)
                self.core_copy(y_lat, k, 0, width)

        def close(self, k):
            if self.has_rest:
                self.take("low", k, 0, self.cut)
                self.core_copy(d_lat, k, 0, self.cut)
                if self.cut < width:
                    self.take("high", k, self.cut, width)
                    self.core_copy(d_lat, k, self.cut, width)

        def finish(self):
            arrived(self.buffer.at[:, :, :, 1 - core], self.core_landed)

    edge_sent = outgoing(fields.at[0, pl.ds(0, 6)])
    edge_landed = {1: landing(), 0: landing()}

    def edges(field):
        landed_at = edge_landed[field % 2]
        send(fields.at[field, 1], fields.at[field, cols + 1], west, edge_sent, landed_at)
        send(fields.at[field, cols], fields.at[field, 0], east, edge_sent, landed_at)

    def last_row(index):
        return lax.rem(index, lat_rows) == lat_rows - 1

    def first_row(index):
        return lax.rem(index, lat_rows) == 0

    take = [
        selector((halo_rows, span), lambda m, n: n == m * lat_rows),
        selector((halo_rows, span), lambda m, n: n == m * lat_rows + lat_rows - 1),
    ]
    for copy in up_load:
        copy.wait()

    @pl.loop(0, chunks)
    def _(c):
        fields[1, pl.ds(1 + c * chunk, chunk)] = up_raw[pl.ds(c * chunk, chunk)].reshape(
            chunk, group_rows, width
        )

    pl.semaphore_wait(barrier, len(greeted))
    edges(1)
    old = Gather(w_old, width, OLD_LINE_TAPS)
    old.line_start()
    old.start_z()
    old.core_copy(lat, 0, 0, width)
    @pl.loop(0, chunks)
    def _(c):
        block = fields[1, pl.ds(1 + c * chunk, chunk)].reshape(span, width)
        for side in range(2):
            halo_out[side, c] = jnp.dot(
                take[side], block, preferred_element_type=jnp.float32
            ).astype(jnp.bfloat16)


    near = chunks - chunks // 2
    has_above, has_below = lat > 0, lat < n_lat - 1
    inner = jnp.logical_and(has_above, has_below)
    outer = jnp.logical_not(inner)
    goes_up = lax.rem(lat, 2) == 1
    parts = (pl.ds(0, near), pl.ds(near, chunks - near))

    x_side = jnp.where(goes_up, 0, 1)
    x_halo = remote(
        halo_out.at[x_side], halo_in.at[x_side], x_peer, outgoing(halo_out.at[0]), landing()
    )
    d_halo = remote(
        halo_out.at[1 - x_side, parts[0]], halo_in.at[1 - x_side, parts[0]], d_peer,
        outgoing(halo_out.at[0, parts[0]], inner), landing(),
    )
    y_halo = remote(
        halo_out.at[1 - x_side, parts[1]], halo_pass, y_peer, outgoing(halo_pass, inner),
        landing(),
    )
    passed = remote(
        halo_pass, halo_in.at[1 - x_side, parts[1]], x_peer, outgoing(halo_pass, outer),
        landing(),
    )

    @pl.when(inner)
    def _():
        y_halo.start()

    x_halo.start()

    @pl.when(inner)
    def _():
        d_halo.start()

    old.line_start_y()
    old.spread_y(0)
    for copy in act_load:
        copy.wait()

    @pl.loop(0, chunks)
    def _(c):
        acts[pl.ds(c * span, span)] = act_raw[pl.ds(c * chunk, chunk)].reshape(span, width)

    part_sent, part_landed = outgoing(part.at[:, :, :, 1 - core]), landing(taps)

    def part_copy(tap):
        return remote(
            part.at[tap, :, :, 1 - core], core_in.at[tap], partner, part_sent,
            part_landed + tap,
        )

    first_sent, second_sent = outgoing(first), outgoing(second)
    third_sent, third_landed = outgoing(last_out), landing()
    first_landed, second_landed = {}, {}

    order = (4, 3, 5, 1, 7, 0, 2, 6, 8)

    def reduce_tap(slot, cut):
        part_copy(slot).wait_recv()
        for k in range(n_q):
            def total(lat_id):
                return part[slot, lat_id, k, core] + core_in[slot, lat_id, k]

            mine[slot, k] = total(lat)
            first[slot, 1, k] = total(d_lat).astype(jnp.bfloat16)
            from_x, from_y = total(x_lat), total(y_lat)
            first[slot, 0, k, :, :cut] = from_y[:, :cut].astype(jnp.bfloat16)
            keep[slot, k, :, :cut] = from_x[:, :cut]
            if cut < width:
                first[slot, 0, k, :, cut:] = from_x[:, cut:].astype(jnp.bfloat16)
                keep[slot, k, :, cut:] = from_y[:, cut:]

    def weight_tap(slot):
        r, s = divmod(order[slot], 3)
        shifted = fields[r, pl.ds(2 - s, cols)].reshape(cols * group_rows, width)
        part[slot] = lax.dot_general(
            acts[...], shifted, (((0,), (0,)), ((), ())), preferred_element_type=jnp.float32,
        ).reshape(n_lat, n_q, 2, rows, width)
        part_copy(slot).start()

    def reduce_first(unit):
        low_slot, high_slot, cut = unit
        piece = pl.ds(low_slot, high_slot - low_slot)
        for slot in (1, 0):
            first_landed[unit, slot] = landing()
            for target, low, high in ((y_peer, 0, cut), (x_peer, cut, width)):
                if low < high:
                    lanes = pl.ds(low, high - low)
                    send(
                        first.at[piece, slot, :, :, lanes],
                        first_in.at[piece, slot, :, :, lanes], target, first_sent,
                        first_landed[unit, slot],
                    )

    def reduce_second(unit):
        low_slot, high_slot, cut = unit
        piece = pl.ds(low_slot, high_slot - low_slot)
        arrived(first_in.at[piece, 1], first_landed[unit, 1])

        @pl.loop(low_slot, high_slot)
        def _(tap):
            for k in range(n_q):
                second[tap, k] = (
                    keep[tap, k] + first_in[tap, 1, k].astype(jnp.float32)
                ).astype(jnp.bfloat16)

        second_landed[unit] = landing()
        for target, low, high in ((x_peer, 0, cut), (y_peer, cut, width)):
            if low < high:
                lanes = pl.ds(low, high - low)
                send(
                    second.at[piece, :, :, lanes], second_in.at[piece, :, :, lanes], target,
                    second_sent, second_landed[unit],
                )

    def reduce_third(unit):
        low_slot, high_slot, _ = unit
        piece = pl.ds(low_slot, high_slot - low_slot)
        arrived(first_in.at[piece, 0], first_landed[unit, 0])
        arrived(second_in.at[piece], second_landed[unit])

        @pl.loop(low_slot, high_slot)
        def _(tap):
            for k in range(n_q):
                block = z_ids[k]
                total = (
                    mine[tap, block] + first_in[tap, 0, block].astype(jnp.float32)
                    + second_in[tap, block].astype(jnp.float32)
                )
                if k == 0:
                    mine[tap, block] = total
                else:
                    last_out[k - 1, tap] = total.astype(jnp.bfloat16)

        for k in range(1, n_q):
            send(
                last_out.at[k - 1, piece], last_in.at[k - 1, piece], z_peers[k - 1],
                third_sent, third_landed,
            )

    def input_piece(index):
        total = None
        for tap in range(taps):
            r, s = divmod(tap, 3)
            shifted = fields[r, pl.ds(index * chunk + 2 - s, chunk)]
            product = lax.dot_general(
                shifted.reshape(span, width), w_old[tap].reshape(-1, width),
                (((1,), (1,)), ((), ())), preferred_element_type=jnp.float32,
            )
            total = product if total is None else total + product
        total = total.reshape(chunk, group_rows, width)
        for b in range(batch):
            input_grad[b, pl.ds(index * chunk, chunk)] = total[
                :, b * lat_rows : (b + 1) * lat_rows
            ].astype(jnp.bfloat16)

    def input_pieces(low, high):
        @pl.loop(low, high)
        def _(index):
            input_piece(index)

    units = [(0, 3, width), (3, 5, half), (5, 7, half), (7, 9, half)]
    weight_tap(0)
    arrived(fields.at[0, pl.ds(0, 2)], edge_landed[1])
    weight_tap(1)
    reduce_tap(0, width)
    weight_tap(2)
    reduce_tap(1, width)
    reduce_tap(2, width)
    reduce_first(units[0])
    @pl.when(outer)
    def _():
        y_halo.wait_recv()
        passed.start()

    old.line_cross()
    old.line_step(1, ("own",))
    x_halo.wait_recv()

    @pl.when(inner)
    def _():
        d_halo.wait_recv()
        passed.wait_recv()

    @pl.when(jnp.logical_not(has_below))
    def _():
        halo_in[0] = jnp.zeros(halo_in.shape[1:], halo_in.dtype)

    @pl.when(jnp.logical_not(has_above))
    def _():
        halo_in[1] = jnp.zeros(halo_in.shape[1:], halo_in.dtype)

    shift = [
        selector((span, span), lambda m, n: jnp.logical_and(n == m + 1, jnp.logical_not(last_row(m)))),
        selector((span, span), lambda m, n: jnp.logical_and(n == m - 1, jnp.logical_not(first_row(m)))),
    ]
    place = [
        selector((span, halo_rows), lambda m, n: jnp.logical_and(n == m // lat_rows, last_row(m))),
        selector((span, halo_rows), lambda m, n: jnp.logical_and(n == m // lat_rows, first_row(m))),
    ]

    @pl.loop(0, chunks)
    def _(c):
        block = fields[1, pl.ds(1 + c * chunk, chunk)].reshape(span, width)
        for side in range(2):
            moved = jnp.dot(shift[side], block, preferred_element_type=jnp.float32)
            moved = moved + jnp.dot(
                place[side], halo_in[side, c], preferred_element_type=jnp.float32
            )
            fields[2 * side, pl.ds(1 + c * chunk, chunk)] = moved.astype(jnp.bfloat16).reshape(
                chunk, group_rows, width
            )

    edges(0)
    edges(2)
    old.line_step(1, ("xy",))
    weight_tap(3)
    weight_tap(4)
    reduce_second(units[0])
    reduce_tap(3, half)
    reduce_tap(4, half)
    reduce_first(units[1])
    arrived(fields.at[0, pl.ds(0, 4)], edge_landed[0])
    weight_tap(5)
    weight_tap(6)
    reduce_tap(5, half)
    reduce_tap(6, half)
    reduce_first(units[2])
    old.line_far()
    old.line_step(2, ("own",))
    weight_tap(7)
    weight_tap(8)
    reduce_tap(7, half)
    reduce_tap(8, half)
    reduce_first(units[3])
    old.line_step(2, ("xy",))
    old.line_step(1, ("d",))
    reduce_second(units[1])
    reduce_third(units[0])
    old.line_step(3, ("own",))
    reduce_second(units[2])
    reduce_third(units[1])
    reduce_second(units[3])
    for k in range(1, n_q):
        old.from_z(k)
        old.spread_y(k)
        old.core_copy(lat, k, 0, width)
    for k in range(n_q):
        old.spread_x(k)
    reduce_third(units[2])
    reduce_third(units[3])
    old.line_step(3, ("xy",))
    old.line_step(2, ("d",))
    for k in range(n_q):
        old.relay_y(k)
        old.relay_x(k)
    arrived(last_in, third_landed)
    square = jnp.zeros((rows, width), jnp.float32)
    for index, tap in enumerate(order):
        grad = mine[index, q]
        for k in range(n_q - 1):
            grad = grad + last_in[k, index].astype(jnp.float32)
        clipped[tap] = grad
        square = square + grad * grad
    square = jnp.sum(square)
    slot = 0
    for stage, peers in enumerate(([partner] + z_peers + z_twins, [x_peer, y_peer, d_peer])):
        norm_out[stage] = jnp.full(norm_out.shape[1:], square, jnp.float32)
        tiles = norm_in.at[pl.ds(slot, len(peers))]
        sent, landed_at = outgoing(tiles), landing()
        for index, target in enumerate(peers):
            send(norm_out.at[stage], norm_in.at[slot + index], target, sent, landed_at)
        arrived(tiles, landed_at)
        tile = norm_out[stage]
        for index in range(len(peers)):
            tile = tile + norm_in[slot + index]
        slot += len(peers)
        square = jnp.max(tile)
    one_load.wait()
    two_load.wait()
    square = jnp.full((1, 1), square, jnp.float32)
    clip_factor = jnp.minimum(1.0, max_norm / (jnp.sqrt(square) + norm_eps))

    @pl.loop(0, taps)
    def _(tap):
        scaled = clip_factor * clipped[tap]
        clipped[tap] = scaled
        moment = beta_one * one[tap] + (1.0 - beta_one) * scaled
        spread = beta_two * two[tap] + (1.0 - beta_two) * scaled * scaled
        new_one[tap] = moment
        new_two[tap] = spread
        first_hat = moment / (1.0 - beta_one**step_count)
        second_hat = spread / (1.0 - beta_two**step_count)
        updated = master[tap] - learn_rate * (
            first_hat / (jnp.sqrt(second_hat) + adam_eps) + decay_rate * master[tap]
        )
        new_master[tap] = updated
        w_new[tap, lat, q, core] = updated.astype(jnp.bfloat16)

    new = Gather(w_new, half, NEW_LINE_TAPS)
    new.line_start()
    new.line_start_y()
    new.start_z()
    new.spread_x(0)
    new.spread_y(0)
    new.core_copy(lat, 0, 0, width)
    old.line_step(3, ("d",))
    for step in range(4, n_q):
        old.line_step(step)
    for k in range(n_q):
        old.close(k)
    old.finish()
    cuts = [chunks * index // (n_q + 2) for index in range(n_q + 3)]
    input_pieces(cuts[0], cuts[1])
    new.line_cross()
    for k in range(1, n_q):
        input_pieces(cuts[k], cuts[k + 1])
        new.from_z(k)
        new.spread_x(k)
        new.spread_y(k)
        new.core_copy(lat, k, 0, width)
        new.relay_x(k - 1)
        new.relay_y(k - 1)
        if k == 1:
            new.line_far()
        new.line_step(k - 1 if k > 1 else n_q)
    input_pieces(cuts[n_q], cuts[n_q + 1])
    new.relay_x(n_q - 1)
    new.relay_y(n_q - 1)
    new.line_step(n_q - 1)
    input_pieces(cuts[n_q + 1], cuts[n_q + 2])
    for k in range(n_q):
        new.close(k)
    new.finish()

    for condition, copy in closing:
        if condition is None:
            copy.wait_send()
        else:
            @pl.when(condition)
            def _(copy=copy):
                copy.wait_send()

    assert used == [send_sem.shape[0], recv_sem.shape[0]]


def land(*refs):
    count = len(refs) // 2
    sources, targets, sem = refs[:count], refs[count : 2 * count], refs[-1]
    copies = [
        pltpu.make_async_copy(source, target, sem.at[index])
        for index, (source, target) in enumerate(zip(sources, targets))
    ]
    for copy in copies:
        copy.start()
    for copy in copies:
        copy.wait()


def landed(arrays):
    anywhere = pl.BlockSpec(memory_space=pl.ANY)
    return pl.pallas_call(
        land,
        out_shape=tuple(jax.ShapeDtypeStruct(a.shape, a.dtype) for a in arrays),
        in_specs=[anywhere] * len(arrays),
        out_specs=(anywhere,) * len(arrays),
        scratch_shapes=[pltpu.SemaphoreType.DMA((len(arrays),))],
        compiler_params=pltpu.CompilerParams(vmem_limit_bytes=1024 * 1024),
        name="land",
    )(*arrays)


def fused_step(up, act, master, one, two):
    n_lat, n_q = lax.axis_size("lat"), lax.axis_size("lon") // 2
    taps, rows, width = master.shape
    batch, cols, lat_rows, _ = up.shape
    group_rows = batch * lat_rows
    chunk = max(c for c in range(1, 17) if cols % c == 0)
    chunks = cols // chunk
    halo_rows = -(-chunk * batch // ROW_TILE) * ROW_TILE
    max_norm = math.sqrt(float(n_lat * n_q * 2 * taps * rows * width))
    bf16, f32 = jnp.bfloat16, jnp.float32
    shard = pltpu.VMEM(master.shape, f32)
    whole = (taps, n_lat, n_q, 2, rows, width)
    lat_block = (taps, n_q, rows, width)
    vmem, hbm = (pl.BlockSpec(memory_space=m) for m in (pltpu.VMEM, pltpu.HBM))
    peers = 2 * n_q + n_lat - 2
    sends, arrivals = 28 + 4 * (n_q - 1), 38 + 9 * n_q + 12 * (n_q - 1)
    return pl.pallas_call(
        functools.partial(whole_step, n_lat, n_q, max_norm),
        out_shape=(
            pltpu.VMEM(up.shape, bf16), pltpu.VMEM(whole, bf16), shard, shard, shard, shard,
        ),
        in_specs=[hbm] * 5,
        out_specs=(vmem,) * 6,
        scratch_shapes=[
            pltpu.VMEM(master.shape, f32),
            pltpu.VMEM(master.shape, f32),
            pltpu.VMEM(master.shape, f32),
            pltpu.VMEM((cols, batch, lat_rows, width), bf16),
            pltpu.VMEM((cols, batch, lat_rows, width), bf16),
            pltpu.VMEM((cols * group_rows, width), bf16),
            pltpu.VMEM((3, cols + 2, group_rows, width), bf16),
            pltpu.VMEM((2, chunks, halo_rows, width), bf16),
            pltpu.VMEM((2, chunks, halo_rows, width), bf16),
            pltpu.VMEM((chunks // 2, halo_rows, width), bf16),
            pltpu.VMEM(whole, bf16),
            pltpu.VMEM(whole, f32),
            pltpu.VMEM((taps, n_lat, n_q, rows, width), f32),
            pltpu.VMEM(lat_block, f32),
            pltpu.VMEM(lat_block, f32),
            pltpu.VMEM((taps, 2, n_q, rows, width), bf16),
            pltpu.VMEM((taps, 2, n_q, rows, width), bf16),
            pltpu.VMEM(lat_block, bf16),
            pltpu.VMEM(lat_block, bf16),
            pltpu.VMEM((n_q - 1, taps, rows, width), bf16),
            pltpu.VMEM((n_q - 1, taps, rows, width), bf16),
            pltpu.VMEM((3, 8, LANE_TILE), f32),
            pltpu.VMEM((peers, 8, LANE_TILE), f32),
            pltpu.SemaphoreType.DMA((2 * batch + 3,)),
            pltpu.SemaphoreType.DMA((sends,)),
            pltpu.SemaphoreType.DMA((arrivals,)),
        ],
        compiler_params=pltpu.CompilerParams(
            collective_id=2, has_side_effects=True, vmem_limit_bytes=48 * 1024 * 1024
        ),
        name="whole_step",
    )(up, act, master, one, two)


def takes_fused(activations, master):
    n_lat, n_q = lax.axis_size("lat"), lax.axis_size("lon") // 2
    batch, lat_rows, cols, _ = activations.shape
    return (
        n_lat == 4 and n_q & (n_q - 1) == 0 and n_q > 1 and master.shape[0] % ROW_TILE == 0
        and (batch * lat_rows) % ROW_TILE == 0 and cols % 2 == 0
        and master.shape[2] % (2 * LANE_TILE) == 0 and master.shape[1] == 9
    )


def per_device(activations, upstream, master, moment_one, moment_two):
    if not takes_fused(activations, master):
        return per_device_general(activations, upstream, master, moment_one, moment_two)

    def by_col(field):
        return jnp.transpose(field, (0, 2, 1, 3))

    def by_tap(array):
        return jnp.transpose(array, (1, 0, 2))

    input_grad, gathered, new_master, new_one, new_two, clipped = landed(fused_step(
        by_col(upstream), by_col(activations), by_tap(master), by_tap(moment_one),
        by_tap(moment_two),
    ))
    new_weights = by_tap(gathered.reshape(gathered.shape[0], -1, gathered.shape[-1]))
    return (
        by_col(input_grad), new_weights, by_tap(new_master), by_tap(new_one), by_tap(new_two),
        by_tap(clipped),
    )


def per_device_general(activations, upstream, master, moment_one, moment_two):
    lat_rows = activations.shape[1]
    lon_cols = activations.shape[2]
    grad_flat = upstream.reshape(-1, upstream.shape[3])
    old_weights = master[:, ::-1].astype(jnp.bfloat16)
    old_full = lax.all_gather(old_weights, ("lat", "lon"), axis=0, tiled=True)
    act_wide, grad_wide = widened((activations, upstream))
    term_maker = input_taps(act_wide, grad_flat, lat_rows, lon_cols)
    partial = term_maker(jnp.int32(0), activations.shape[3])

    def by_tap(array):
        return jnp.transpose(array, (1, 0, 2))

    gathered, new_master, new_one, new_two, clipped = fused_update(
        by_tap(partial), by_tap(master), by_tap(moment_one), by_tap(moment_two)
    )
    new_weights = jnp.transpose(gathered, (2, 1, 0, 4, 3, 5)).reshape(
        activations.shape[3], gathered.shape[3], gathered.shape[5]
    )
    old_full, new_one = lax.optimization_barrier((old_full, new_one))
    input_grad = lax.conv_general_dilated(
        grad_wide,
        old_full.reshape(old_full.shape[0], 3, 3, old_full.shape[2]),
        (1, 1),
        "VALID",
        dimension_numbers=("NHWC", "OHWI", "NHWC"),
        preferred_element_type=jnp.float32,
    ).astype(jnp.bfloat16)
    return (
        input_grad, new_weights, by_tap(new_master), by_tap(new_one), by_tap(new_two),
        by_tap(clipped),
    )


def solution(mesh):
    in_specs = (
        P(None, "lat", "lon", None),
        P(None, "lat", "lon", None),
        P(("lat", "lon"), None, None),
        P(("lat", "lon"), None, None),
        P(("lat", "lon"), None, None),
    )
    out_specs = (
        P(None, "lat", "lon", None),
        P(),
        P(("lat", "lon"), None, None),
        P(("lat", "lon"), None, None),
        P(("lat", "lon"), None, None),
        P(("lat", "lon"), None, None),
    )
    return jax.shard_map(
        per_device, mesh=mesh, in_specs=in_specs, out_specs=out_specs, check_vma=False
    )
```

```python
import functools
import math

import jax
import jax.numpy as jnp
from jax import lax
from jax.experimental import pallas as pl
from jax.experimental.pallas import tpu as pltpu
from jax.sharding import PartitionSpec as P

MESH = pl.DeviceIdType.MESH

CIN = 512
COUT = 512
TAPS = 9


learn_rate = 0.01
beta_one = 0.9
beta_two = 0.999
adam_eps = 1e-08
decay_rate = 0.1
step_count = 10.0
norm_eps = 1e-06


def halo_kernel(n_lat, n_lon, *refs):
    sources, landings, (send_sem, recv_sem) = refs[:8], refs[8:16], refs[16:]
    lat, lon = lax.axis_index("lat"), lax.axis_index("lon")
    steps = ((-1, 0), (1, 0), (0, -1), (0, 1), (-1, -1), (-1, 1), (1, -1), (1, 1))
    targets = [
        (lax.rem(lat + dy + n_lat, n_lat), lax.rem(lon + dx + n_lon, n_lon)) for dy, dx in steps
    ]
    barrier = pltpu.get_barrier_semaphore()
    for target in targets:
        pl.semaphore_signal(barrier, inc=1, device_id=target, device_id_type=MESH)
    pl.semaphore_wait(barrier, len(targets))
    copies = []
    for index, target in enumerate(targets):
        copy = pltpu.make_async_remote_copy(
            src_ref=sources[index], dst_ref=landings[index], send_sem=send_sem.at[index],
            recv_sem=recv_sem.at[index], device_id=target, device_id_type=MESH,
        )
        copy.start()
        copies.append(copy)
    for copy in copies:
        copy.wait()


def widened(fields):
    both = jnp.stack(fields)
    top, bottom = both[:, :, 0], both[:, :, -1]
    pieces = (
        top, bottom, both[:, :, :, 0], both[:, :, :, -1],
        top[:, :, 0], top[:, :, -1], bottom[:, :, 0], bottom[:, :, -1],
    )
    landed = pl.pallas_call(
        functools.partial(halo_kernel, lax.axis_size("lat"), lax.axis_size("lon")),
        out_shape=tuple(jax.ShapeDtypeStruct(p.shape, p.dtype) for p in pieces),
        in_specs=[pl.BlockSpec(memory_space=pltpu.VMEM)] * 8,
        out_specs=(pl.BlockSpec(memory_space=pltpu.VMEM),) * 8,
        scratch_shapes=[pltpu.SemaphoreType.DMA((8,)), pltpu.SemaphoreType.DMA((8,))],
        compiler_params=pltpu.CompilerParams(
            collective_id=1, has_side_effects=True, vmem_limit_bytes=24 * 1024 * 1024
        ),
        name="halo",
    )(*pieces)
    below, above, east, west, below_east, below_west, above_east, above_west = landed

    def row(start, middle, end):
        return jnp.concatenate([start[:, None, None], middle[:, None], end[:, None, None]], axis=2)

    wide = []
    for index, field in enumerate(fields):
        middle = jnp.concatenate(
            [west[index][:, :, None], field, east[index][:, :, None]], axis=2
        )
        first = row(above_west[index], above[index], above_east[index])
        last = row(below_west[index], below[index], below_east[index])
        wide.append(mask_poles(jnp.concatenate([first, middle, last], axis=1)))
    return wide


def mask_poles(wide_field):
    lat_index = lax.axis_index("lat")
    lat_count = lax.axis_size("lat")
    total_rows = wide_field.shape[1]
    row_ids = lax.broadcasted_iota(jnp.int32, (1, total_rows, 1, 1), 1)
    upper = jnp.logical_and(row_ids == 0, lat_index == 0)
    lower = jnp.logical_and(row_ids == total_rows - 1, lat_index == lat_count - 1)
    return jnp.where(jnp.logical_or(upper, lower), jnp.zeros((), wide_field.dtype), wide_field)


def input_taps(act_wide, grad_flat, lat_rows, lon_cols):

    def input_compute(first_row, row_count):
        tap_parts = []
        for tap_index in range(9):
            row_off, col_off = divmod(tap_index, 3)
            tap_slab = act_wide[
                :, row_off : row_off + lat_rows, col_off : col_off + lon_cols, :
            ].reshape(-1, row_count)
            tap_parts.append(
                lax.dot_general(
                    tap_slab,
                    grad_flat,
                    (((0,), (0,)), ((), ())),
                    preferred_element_type=jnp.float32,
                )
            )
        return jnp.stack(tap_parts, axis=1)

    return input_compute


def reduce_update_gather(
    n_lat, n_q, max_norm, part, master, one, two,
    gathered, new_master, new_one, new_two, clipped,
    core_in, sums, right_in, left_in, lat_out, lat_in, norm_out, norm_in,
    send_sem, recv_sem,
):
    lat = lax.axis_index("lat")
    lon = lax.axis_index("lon")
    core = lax.rem(lon, 2)
    q = lon // 2
    hops = n_q // 2
    half = n_lat // 2
    counter = [0]
    pending = []

    def at(lat_id, q_id, core_id):
        return (lat_id, q_id * 2 + core_id)

    partner = at(lat, q, 1 - core)
    right_q = lax.rem(q + 1, n_q)
    left_q = lax.rem(q + n_q - 1, n_q)
    right, left = at(lat, right_q, core), at(lat, left_q, core)
    q_peers = [at(lat, lax.rem(q + d, n_q), core) for d in range(1, n_q)]
    lat_peers = [at(lax.rem(lat + d, n_lat), q, core) for d in range(1, n_lat)]

    def send(src, dst, target):
        index = counter[0]
        counter[0] += 1
        copy = pltpu.make_async_remote_copy(
            src_ref=src, dst_ref=dst, send_sem=send_sem.at[index],
            recv_sem=recv_sem.at[index], device_id=target, device_id_type=MESH,
        )
        copy.start()
        pending.append(copy)
        return copy

    def wrap(index, size):
        return lax.rem(index + size, size)

    barrier = pltpu.get_barrier_semaphore()
    greeted = [partner] + q_peers + lat_peers
    for device in greeted:
        pl.semaphore_signal(barrier, inc=1, device_id=device, device_id_type=MESH)
    pl.semaphore_wait(barrier, len(greeted))

    order = []
    for step in range(hops):
        for block in (hops - step, -hops + step):
            if block % n_q not in order:
                order.append(block % n_q)
    order.append(0)
    core_copies = []
    for offset in order:
        block = lax.rem(q + offset, n_q)
        core_copies.append(
            send(part.at[:, :, block, 1 - core], core_in.at[:, :, block], partner)
        )
    arrived = {}

    def core_sum(offset):
        if offset in arrived:
            return
        arrived[offset] = True
        core_copies[order.index(offset)].wait_recv()
        block = lax.rem(q + offset, n_q)

        @pl.loop(0, n_lat)
        def _(row):
            sums[block, row] = (
                part[:, row, block, core] + core_in[:, row, block]
            ).astype(jnp.bfloat16)

    def add_into(block, low, high, source):
        @pl.loop(low, high)
        def _(row):
            sums[block, row] = (
                sums[block, row].astype(jnp.float32) + source[row].astype(jnp.float32)
            ).astype(jnp.bfloat16)

    ring = []
    for step in range(hops):
        right_off = (hops - step) % n_q
        left_off = (step - hops) % n_q
        core_sum(right_off)
        core_sum(left_off)
        right_block = lax.rem(q + right_off, n_q)
        left_block = lax.rem(q + left_off, n_q)
        if step == 0:
            ring.append((
                send(sums.at[right_block, pl.ds(0, half)], right_in.at[0, pl.ds(0, half)], right),
                send(sums.at[left_block, pl.ds(half, n_lat - half)],
                     left_in.at[0, pl.ds(half, n_lat - half)], left),
            ))
        else:
            from_left, from_right = ring[-1]
            bounds = (0, half, half, n_lat) if step == 1 else (0, n_lat, 0, n_lat)
            from_left.wait_recv()
            add_into(right_block, bounds[0], bounds[1], right_in.at[step - 1])
            going_right = send(sums.at[right_block], right_in.at[step], right)
            from_right.wait_recv()
            add_into(left_block, bounds[2], bounds[3], left_in.at[step - 1])
            ring.append((going_right, send(sums.at[left_block], left_in.at[step], left)))
    core_sum(0)
    for copy in ring[-1]:
        copy.wait_recv()

    def q_total(row):
        total = part[:, row, q, core] + core_in[:, row, q]
        if hops > 1:
            return (
                total + right_in[hops - 1, row].astype(jnp.float32)
                + left_in[hops - 1, row].astype(jnp.float32)
            )
        return total + jnp.where(
            row < half, right_in[0, row].astype(jnp.float32), left_in[0, row].astype(jnp.float32)
        )

    lat_copies = []
    for step in range(1, n_lat):
        target = lax.rem(lat + step, n_lat)
        lat_out[step - 1] = q_total(target).astype(jnp.bfloat16)
        lat_copies.append(send(lat_out.at[step - 1], lat_in.at[step - 1], lat_peers[step - 1]))
    grad = q_total(lat)
    for step, copy in enumerate(lat_copies):
        copy.wait_recv()
        grad = grad + lat_in[step].astype(jnp.float32)
    clipped[...] = grad

    square = jnp.sum(grad * grad)
    slot = 0
    for stage, peers in enumerate(([partner], q_peers, lat_peers)):
        norm_out[stage] = jnp.full(norm_out.shape[1:], square, jnp.float32)
        copies = []
        for target in peers:
            copies.append(send(norm_out.at[stage], norm_in.at[slot], target))
            slot += 1
        tile = norm_out[stage]
        for index, copy in enumerate(copies):
            copy.wait_recv()
            tile = tile + norm_in[slot - len(peers) + index]
        square = jnp.max(tile)
    square = jnp.full((1, 1), square, jnp.float32)
    clip_factor = jnp.minimum(1.0, max_norm / (jnp.sqrt(square) + norm_eps))

    @pl.loop(0, clipped.shape[0])
    def _(tap):
        scaled = clip_factor * clipped[tap]
        clipped[tap] = scaled
        first = beta_one * one[tap] + (1.0 - beta_one) * scaled
        second = beta_two * two[tap] + (1.0 - beta_two) * scaled * scaled
        new_one[tap] = first
        new_two[tap] = second
        first_hat = first / (1.0 - beta_one**step_count)
        second_hat = second / (1.0 - beta_two**step_count)
        updated = master[tap] - learn_rate * (
            first_hat / (jnp.sqrt(second_hat) + adam_eps) + decay_rate * master[tap]
        )
        new_master[tap] = updated
        gathered[core, q, lat, tap] = updated.astype(jnp.bfloat16)

    copies = [
        send(gathered.at[core, q, lat], gathered.at[core, q, lat], peer) for peer in lat_peers
    ]
    for copy in copies:
        copy.wait_recv()
    core_in_copies = []

    def to_partner(block, low, count):
        piece = gathered.at[core, block, pl.ds(low, count)]
        core_in_copies.append(send(piece, piece, partner))

    from_left = from_right = None
    for step in range(hops):
        last = step == hops - 1
        right_block = wrap(q - step, n_q)
        left_block = lax.rem(q + step, n_q)
        if from_left is not None:
            from_left.wait_recv()
        piece = gathered.at[core, right_block, pl.ds(0, half if last else n_lat)]
        going_right = send(piece, piece, right)
        if from_right is not None:
            from_right.wait_recv()
        low = half if last else 0
        piece = gathered.at[core, left_block, pl.ds(low, n_lat - low)]
        going_left = send(piece, piece, left)
        to_partner(right_block, 0, n_lat)
        if step > 0:
            to_partner(left_block, 0, n_lat)
        from_left, from_right = going_right, going_left
    far = lax.rem(q + hops, n_q)
    from_left.wait_recv()
    to_partner(far, 0, half)
    from_right.wait_recv()
    to_partner(far, half, n_lat - half)
    for copy in core_in_copies:
        copy.wait_recv()
    for copy in pending:
        copy.wait_send()


def fused_update(partial, master, one, two):
    n_lat, n_q = lax.axis_size("lat"), lax.axis_size("lon") // 2
    taps, rows, width = master.shape
    part = partial.reshape(taps, n_lat, n_q, 2, rows, width)
    max_norm = math.sqrt(float(partial.size))
    shard = jax.ShapeDtypeStruct(master.shape, jnp.float32)
    hops = n_q // 2
    half_type = jnp.bfloat16
    block = (n_lat, taps, rows, width)
    peers = n_q + n_lat - 1
    vmem = pl.BlockSpec(memory_space=pltpu.VMEM)
    copies = 64 + 8 * (n_q + n_lat)
    return pl.pallas_call(
        functools.partial(reduce_update_gather, n_lat, n_q, max_norm),
        out_shape=(
            jax.ShapeDtypeStruct((2, n_q) + block, half_type), shard, shard, shard, shard,
        ),
        in_specs=[vmem] * 4,
        out_specs=(vmem,) * 5,
        scratch_shapes=[
            pltpu.VMEM((taps, n_lat, n_q, rows, width), jnp.float32),
            pltpu.VMEM((n_q,) + block, half_type),
            pltpu.VMEM((hops,) + block, half_type),
            pltpu.VMEM((hops,) + block, half_type),
            pltpu.VMEM((n_lat - 1, taps, rows, width), half_type),
            pltpu.VMEM((n_lat - 1, taps, rows, width), half_type),
            pltpu.VMEM((3, 8, 128), jnp.float32),
            pltpu.VMEM((peers, 8, 128), jnp.float32),
            pltpu.SemaphoreType.DMA((copies,)),
            pltpu.SemaphoreType.DMA((copies,)),
        ],
        compiler_params=pltpu.CompilerParams(
            collective_id=0, has_side_effects=True, vmem_limit_bytes=60 * 1024 * 1024
        ),
        name="reduce_update_gather",
    )(part, master, one, two)


LANE_TILE = 128
ROW_TILE = 16
OLD_LINE_TAPS = 5
NEW_LINE_TAPS = 2


def selector(shape, rows_of):
    rows = lax.broadcasted_iota(jnp.int32, shape, 0)
    cols = lax.broadcasted_iota(jnp.int32, shape, 1)
    return jnp.where(rows_of(rows, cols), 1.0, 0.0).astype(jnp.bfloat16)


def whole_step(
    n_lat, n_q, max_norm,
    up_hbm, act_hbm, master_hbm, one_hbm, two_hbm,
    input_grad, w_new, new_master, new_one, new_two, clipped,
    master, one, two, up_raw, act_raw, acts, fields, halo_out, halo_in, halo_pass, w_old, part, core_in, mine, keep,
    first, first_in, second, second_in, last_out, last_in,
    norm_out, norm_in, load_sem, send_sem, recv_sem,
):
    lat = lax.axis_index("lat")
    lon = lax.axis_index("lon")
    n_lon = n_q * 2
    core = lax.rem(lon, 2)
    q = lon // 2
    taps, rows, width = master.shape
    cols, batch, lat_rows, _ = up_raw.shape
    group_rows = batch * lat_rows
    chunks, halo_rows = halo_out.shape[1], halo_out.shape[2]
    chunk = cols // chunks
    span = chunk * group_rows
    half = width // 2

    def at(lat_id, q_id, core_id):
        return (lat_id, q_id * 2 + core_id)

    x_lat = lat + 1 - 2 * lax.rem(lat, 2)
    y_lat = lax.rem(lat + 2, 4)
    d_lat = x_lat + y_lat - lat
    partner = at(lat, q, 1 - core)
    x_peer, y_peer, d_peer = at(x_lat, q, core), at(y_lat, q, core), at(d_lat, q, core)

    def across(k):
        flipped = q
        bit = 1
        while bit < n_q:
            if k & bit:
                flipped = flipped + bit - 2 * bit * lax.rem(flipped // bit, 2)
            bit *= 2
        return flipped

    z_ids = [across(k) for k in range(n_q)]
    z_peers = [at(lat, z_ids[k], core) for k in range(1, n_q)]
    next_z, last_z = at(lat, jnp.minimum(q + 1, n_q - 1), core), at(lat, jnp.maximum(q - 1, 0), core)
    z_twins = [at(lat, z_ids[k], 1 - core) for k in range(1, n_q)]
    west = (lat, lax.rem(lon + n_lon - 1, n_lon))
    east = (lat, lax.rem(lon + 1, n_lon))
    above = (jnp.maximum(lat - 1, 0), lon)
    below = (jnp.minimum(lat + 1, n_lat - 1), lon)

    used = [0, 0]
    closing = []

    def remote(src, dst, target, sent, landed_at):
        return pltpu.make_async_remote_copy(
            src_ref=src, dst_ref=dst, send_sem=send_sem.at[sent],
            recv_sem=recv_sem.at[landed_at], device_id=target, device_id_type=MESH,
        )

    def landing(count=1):
        used[1] += count
        return used[1] - count

    def outgoing(view, condition=None):
        used[0] += 1
        closing.append((condition, remote(view, view, partner, used[0] - 1, 0)))
        return used[0] - 1

    def arrived(view, landed_at):
        remote(view, view, partner, 0, landed_at).wait_recv()

    def send(src, dst, target, sent, landed_at):
        remote(src, dst, target, sent, landed_at).start()

    barrier = pltpu.get_barrier_semaphore()
    greeted = [partner, x_peer, y_peer, d_peer] + z_peers + z_twins
    for device in greeted:
        pl.semaphore_signal(barrier, inc=1, device_id=device, device_id_type=MESH)

    def load(source, target, base):
        copies = [
            pltpu.make_async_copy(source.at[b], target.at[:, b], load_sem.at[base + b])
            for b in range(batch)
        ]
        for copy in copies:
            copy.start()
        return copies

    def load_whole(source, target, index):
        copy = pltpu.make_async_copy(source, target, load_sem.at[index])
        copy.start()
        return copy

    master_load = load_whole(master_hbm, master, 2 * batch)
    up_load, act_load = load(up_hbm, up_raw, 0), load(act_hbm, act_raw, batch)
    one_load = load_whole(one_hbm, one, 2 * batch + 1)
    two_load = load_whole(two_hbm, two, 2 * batch + 2)
    master_load.wait()
    for tap in range(taps):
        w_old[tap, lat, q, core] = master[tap].astype(jnp.bfloat16)

    class Gather:
        def __init__(self, buffer, cut, line_taps):
            self.buffer, self.cut, self.line_taps = buffer, cut, line_taps
            self.line = pl.ds(0, line_taps)
            self.rest = pl.ds(line_taps, taps - line_taps)
            self.has_rest = line_taps < taps
            self.core_sent = outgoing(buffer.at[:, :, :, core])
            self.core_landed = landing()
            self.sent, self.landed = {}, {}
            if self.has_rest:
                for name, view in (
                    ("z", buffer.at[self.rest, lat, pl.ds(0, n_q - 1), core]),
                    ("x", buffer.at[self.rest, lat, :, core]),
                    ("y", buffer.at[self.rest, lat, :, core]),
                    ("low", buffer.at[self.rest, x_lat, :, core, :, pl.ds(0, cut)]),
                ):
                    self.sent[name], self.landed[name] = outgoing(view), landing(n_q)
                if cut < width:
                    lanes = pl.ds(cut, width - cut)
                    self.sent["high"] = outgoing(
                        buffer.at[self.rest, y_lat, :, core, :, lanes]
                    )
                    self.landed["high"] = landing(n_q)
            if line_taps:
                for name in ("line_x", "line_y", "line_d"):
                    self.sent[name] = outgoing(self.line_block(lat, q))
                    self.landed[name] = landing()
                for step in range(n_q - 1):
                    plane = buffer.at[self.line, :, q, core]
                    self.sent["up", step] = outgoing(
                        plane, jnp.logical_and(q >= step, q < n_q - 1)
                    )
                    self.sent["down", step] = outgoing(
                        plane, jnp.logical_and(q < n_q - step, q > 0)
                    )
                    for name in ("own", "xy", "d"):
                        self.landed["up", name, step + 1] = landing()
                        self.landed["down", name, step + 1] = landing()

        def block(self, lat_id, q_id, low, high):
            return self.buffer.at[
                self.rest, lat_id, q_id, core, :, pl.ds(low, high - low)
            ]

        def give(self, name, k, lat_id, q_id, low, high, target):
            piece = self.block(lat_id, q_id, low, high)
            send(piece, piece, target, self.sent[name], self.landed[name] + k)

        def take(self, name, k, low, high):
            arrived(self.block(lat, q, low, high), self.landed[name] + k)

        def core_copy(self, lat_id, k, low, high):
            if self.has_rest:
                piece = self.block(lat_id, z_ids[k], low, high)
                send(piece, piece, partner, self.core_sent, self.core_landed)

        def line_block(self, lat_id, q_id):
            return self.buffer.at[self.line, lat_id, q_id, core]

        def line_give(self, name, lat_id, target):
            piece = self.line_block(lat_id, q)
            send(piece, piece, target, self.sent[name], self.landed[name])

        def line_take(self, name):
            arrived(self.line_block(lat, q), self.landed[name])

        def line_core(self, lat_id, q_id):
            piece = self.line_block(lat_id, q_id)
            send(piece, piece, partner, self.core_sent, self.core_landed)

        def line_pass(self, name, lat_ids, step):
            for way, here, ahead, block, target in (
                ("up", q >= step, q < n_q - 1, jnp.maximum(q - step, 0), next_z),
                ("down", q < n_q - step, q > 0, jnp.minimum(q + step, n_q - 1), last_z),
            ):
                if step:
                    @pl.when(here)
                    def _():
                        view = self.buffer.at[self.line, pl.ds(0, len(lat_ids)), q, core]
                        arrived(view, self.landed[way, name, step])
                        for lat_id in lat_ids:
                            self.line_core(lat_id, block)

                if step < n_q - 1:
                    @pl.when(jnp.logical_and(here, ahead))
                    def _():
                        for lat_id in lat_ids:
                            piece = self.line_block(lat_id, block)
                            send(
                                piece, piece, target, self.sent[way, step],
                                self.landed[way, name, step + 1],
                            )

        def line_step(self, step, names=("own", "xy", "d")):
            if not self.line_taps or step >= n_q:
                return
            for name in names:
                lat_ids = {"own": (lat,), "xy": (x_lat, y_lat), "d": (d_lat,)}[name]
                self.line_pass(name, lat_ids, step)

        def line_start(self):
            if self.line_taps:
                self.line_give("line_x", lat, x_peer)
                self.line_step(0, ("own",))
                self.line_core(lat, q)

        def line_start_y(self):
            if self.line_taps:
                self.line_give("line_y", lat, y_peer)

        def line_cross(self):
            if self.line_taps:
                self.line_take("line_x")
                self.line_give("line_d", x_lat, y_peer)
                self.line_core(x_lat, q)
                self.line_take("line_y")
                self.line_core(y_lat, q)
                self.line_step(0, ("xy",))

        def line_far(self):
            if self.line_taps:
                self.line_take("line_d")
                self.line_core(d_lat, q)
                self.line_step(0, ("d",))

        def start_z(self):
            if self.has_rest:
                for k in range(1, n_q):
                    self.give("z", k, lat, q, 0, width, z_peers[k - 1])

        def spread_x(self, k):
            if self.has_rest:
                self.give("x", k, lat, z_ids[k], 0, width, x_peer)

        def spread_y(self, k):
            if self.has_rest:
                self.give("y", k, lat, z_ids[k], 0, width, y_peer)

        def from_z(self, k):
            if self.has_rest:
                self.take("z", k, 0, width)

        def relay_x(self, k):
            if self.has_rest:
                self.take("x", k, 0, width)
                self.give("low", k, x_lat, z_ids[k], 0, self.cut, y_peer)
                self.core_copy(x_lat, k, 0, width)

        def relay_y(self, k):
            if self.has_rest:
                self.take("y", k, 0, width)
                if self.cut < width:
                    self.give("high", k, y_lat, z_ids[k], self.cut, width, x_peer)
                self.core_copy(y_lat, k, 0, width)

        def close(self, k):
            if self.has_rest:
                self.take("low", k, 0, self.cut)
                self.core_copy(d_lat, k, 0, self.cut)
                if self.cut < width:
                    self.take("high", k, self.cut, width)
                    self.core_copy(d_lat, k, self.cut, width)

        def finish(self):
            arrived(self.buffer.at[:, :, :, 1 - core], self.core_landed)

    edge_sent = outgoing(fields.at[0, pl.ds(0, 6)])
    edge_landed = {1: landing(), 0: landing()}

    def edges(field):
        landed_at = edge_landed[field % 2]
        send(fields.at[field, 1], fields.at[field, cols + 1], west, edge_sent, landed_at)
        send(fields.at[field, cols], fields.at[field, 0], east, edge_sent, landed_at)

    def last_row(index):
        return lax.rem(index, lat_rows) == lat_rows - 1

    def first_row(index):
        return lax.rem(index, lat_rows) == 0

    take = [
        selector((halo_rows, span), lambda m, n: n == m * lat_rows),
        selector((halo_rows, span), lambda m, n: n == m * lat_rows + lat_rows - 1),
    ]
    for copy in up_load:
        copy.wait()

    @pl.loop(0, chunks)
    def _(c):
        fields[1, pl.ds(1 + c * chunk, chunk)] = up_raw[pl.ds(c * chunk, chunk)].reshape(
            chunk, group_rows, width
        )

    pl.semaphore_wait(barrier, len(greeted))
    edges(1)
    old = Gather(w_old, width, OLD_LINE_TAPS)
    old.line_start()
    old.start_z()
    old.core_copy(lat, 0, 0, width)
    @pl.loop(0, chunks)
    def _(c):
        block = fields[1, pl.ds(1 + c * chunk, chunk)].reshape(span, width)
        for side in range(2):
            halo_out[side, c] = jnp.dot(
                take[side], block, preferred_element_type=jnp.float32
            ).astype(jnp.bfloat16)


    near = chunks - chunks // 2
    has_above, has_below = lat > 0, lat < n_lat - 1
    inner = jnp.logical_and(has_above, has_below)
    outer = jnp.logical_not(inner)
    goes_up = lax.rem(lat, 2) == 1
    parts = (pl.ds(0, near), pl.ds(near, chunks - near))

    x_side = jnp.where(goes_up, 0, 1)
    x_halo = remote(
        halo_out.at[x_side], halo_in.at[x_side], x_peer, outgoing(halo_out.at[0]), landing()
    )
    d_halo = remote(
        halo_out.at[1 - x_side, parts[0]], halo_in.at[1 - x_side, parts[0]], d_peer,
        outgoing(halo_out.at[0, parts[0]], inner), landing(),
    )
    y_halo = remote(
        halo_out.at[1 - x_side, parts[1]], halo_pass, y_peer, outgoing(halo_pass, inner),
        landing(),
    )
    passed = remote(
        halo_pass, halo_in.at[1 - x_side, parts[1]], x_peer, outgoing(halo_pass, outer),
        landing(),
    )

    @pl.when(inner)
    def _():
        y_halo.start()

    x_halo.start()

    @pl.when(inner)
    def _():
        d_halo.start()

    old.line_start_y()
    old.spread_y(0)
    for copy in act_load:
        copy.wait()

    @pl.loop(0, chunks)
    def _(c):
        acts[pl.ds(c * span, span)] = act_raw[pl.ds(c * chunk, chunk)].reshape(span, width)

    part_sent, part_landed = outgoing(part.at[:, :, :, 1 - core]), landing(taps)

    def part_copy(tap):
        return remote(
            part.at[tap, :, :, 1 - core], core_in.at[tap], partner, part_sent,
            part_landed + tap,
        )

    first_sent, second_sent = outgoing(first), outgoing(second)
    third_sent, third_landed = outgoing(last_out), landing()
    first_landed, second_landed = {}, {}

    order = (4, 3, 5, 1, 7, 0, 2, 6, 8)

    def reduce_tap(slot, cut):
        part_copy(slot).wait_recv()
        for k in range(n_q):
            def total(lat_id):
                return part[slot, lat_id, k, core] + core_in[slot, lat_id, k]

            mine[slot, k] = total(lat)
            first[slot, 1, k] = total(d_lat).astype(jnp.bfloat16)
            from_x, from_y = total(x_lat), total(y_lat)
            first[slot, 0, k, :, :cut] = from_y[:, :cut].astype(jnp.bfloat16)
            keep[slot, k, :, :cut] = from_x[:, :cut]
            if cut < width:
                first[slot, 0, k, :, cut:] = from_x[:, cut:].astype(jnp.bfloat16)
                keep[slot, k, :, cut:] = from_y[:, cut:]

    def weight_tap(slot):
        r, s = divmod(order[slot], 3)
        shifted = fields[r, pl.ds(2 - s, cols)].reshape(cols * group_rows, width)
        part[slot] = lax.dot_general(
            acts[...], shifted, (((0,), (0,)), ((), ())), preferred_element_type=jnp.float32,
        ).reshape(n_lat, n_q, 2, rows, width)
        part_copy(slot).start()

    def reduce_first(unit):
        low_slot, high_slot, cut = unit
        piece = pl.ds(low_slot, high_slot - low_slot)
        for slot in (1, 0):
            first_landed[unit, slot] = landing()
            for target, low, high in ((y_peer, 0, cut), (x_peer, cut, width)):
                if low < high:
                    lanes = pl.ds(low, high - low)
                    send(
                        first.at[piece, slot, :, :, lanes],
                        first_in.at[piece, slot, :, :, lanes], target, first_sent,
                        first_landed[unit, slot],
                    )

    def reduce_second(unit):
        low_slot, high_slot, cut = unit
        piece = pl.ds(low_slot, high_slot - low_slot)
        arrived(first_in.at[piece, 1], first_landed[unit, 1])

        @pl.loop(low_slot, high_slot)
        def _(tap):
            for k in range(n_q):
                second[tap, k] = (
                    keep[tap, k] + first_in[tap, 1, k].astype(jnp.float32)
                ).astype(jnp.bfloat16)

        second_landed[unit] = landing()
        for target, low, high in ((x_peer, 0, cut), (y_peer, cut, width)):
            if low < high:
                lanes = pl.ds(low, high - low)
                send(
                    second.at[piece, :, :, lanes], second_in.at[piece, :, :, lanes], target,
                    second_sent, second_landed[unit],
                )

    def reduce_third(unit):
        low_slot, high_slot, _ = unit
        piece = pl.ds(low_slot, high_slot - low_slot)
        arrived(first_in.at[piece, 0], first_landed[unit, 0])
        arrived(second_in.at[piece], second_landed[unit])

        @pl.loop(low_slot, high_slot)
        def _(tap):
            for k in range(n_q):
                block = z_ids[k]
                total = (
                    mine[tap, block] + first_in[tap, 0, block].astype(jnp.float32)
                    + second_in[tap, block].astype(jnp.float32)
                )
                if k == 0:
                    mine[tap, block] = total
                else:
                    last_out[k - 1, tap] = total.astype(jnp.bfloat16)

        for k in range(1, n_q):
            send(
                last_out.at[k - 1, piece], last_in.at[k - 1, piece], z_peers[k - 1],
                third_sent, third_landed,
            )

    def input_piece(index):
        total = None
        for tap in range(taps):
            r, s = divmod(tap, 3)
            shifted = fields[r, pl.ds(index * chunk + 2 - s, chunk)]
            product = lax.dot_general(
                shifted.reshape(span, width), w_old[tap].reshape(-1, width),
                (((1,), (1,)), ((), ())), preferred_element_type=jnp.float32,
            )
            total = product if total is None else total + product
        total = total.reshape(chunk, group_rows, width)
        for b in range(batch):
            input_grad[b, pl.ds(index * chunk, chunk)] = total[
                :, b * lat_rows : (b + 1) * lat_rows
            ].astype(jnp.bfloat16)

    def input_pieces(low, high):
        @pl.loop(low, high)
        def _(index):
            input_piece(index)

    units = [(0, 3, width), (3, 5, half), (5, 7, half), (7, 9, half)]
    weight_tap(0)
    arrived(fields.at[0, pl.ds(0, 2)], edge_landed[1])
    weight_tap(1)
    reduce_tap(0, width)
    weight_tap(2)
    reduce_tap(1, width)
    reduce_tap(2, width)
    reduce_first(units[0])
    @pl.when(outer)
    def _():
        y_halo.wait_recv()
        passed.start()

    old.line_cross()
    old.line_step(1, ("own",))
    shift = [
        selector((span, span), lambda m, n: jnp.logical_and(n == m + 1, jnp.logical_not(last_row(m)))),
        selector((span, span), lambda m, n: jnp.logical_and(n == m - 1, jnp.logical_not(first_row(m)))),
    ]
    place = [
        selector((span, halo_rows), lambda m, n: jnp.logical_and(n == m // lat_rows, last_row(m))),
        selector((span, halo_rows), lambda m, n: jnp.logical_and(n == m // lat_rows, first_row(m))),
    ]

    @pl.loop(0, chunks)
    def _(c):
        block = fields[1, pl.ds(1 + c * chunk, chunk)].reshape(span, width)
        for side in range(2):
            moved = jnp.dot(shift[side], block, preferred_element_type=jnp.float32)
            fields[2 * side, pl.ds(1 + c * chunk, chunk)] = moved.astype(jnp.bfloat16).reshape(
                chunk, group_rows, width
            )

    x_halo.wait_recv()

    @pl.when(inner)
    def _():
        d_halo.wait_recv()
        passed.wait_recv()

    @pl.when(jnp.logical_not(has_below))
    def _():
        halo_in[0] = jnp.zeros(halo_in.shape[1:], halo_in.dtype)

    @pl.when(jnp.logical_not(has_above))
    def _():
        halo_in[1] = jnp.zeros(halo_in.shape[1:], halo_in.dtype)

    @pl.loop(0, chunks)
    def _(c):
        for side in range(2):
            piece = pl.ds(1 + c * chunk, chunk)
            placed = jnp.dot(place[side], halo_in[side, c], preferred_element_type=jnp.float32)
            inside = fields[2 * side, piece].reshape(span, width).astype(jnp.float32)
            fields[2 * side, piece] = (inside + placed).astype(jnp.bfloat16).reshape(
                chunk, group_rows, width
            )

    edges(0)
    edges(2)
    old.line_step(1, ("xy",))
    weight_tap(3)
    weight_tap(4)
    reduce_second(units[0])
    reduce_tap(3, half)
    reduce_tap(4, half)
    reduce_first(units[1])
    arrived(fields.at[0, pl.ds(0, 4)], edge_landed[0])
    weight_tap(5)
    weight_tap(6)
    reduce_tap(5, half)
    reduce_tap(6, half)
    reduce_first(units[2])
    old.line_far()
    old.line_step(2, ("own",))
    weight_tap(7)
    weight_tap(8)
    reduce_tap(7, half)
    reduce_tap(8, half)
    reduce_first(units[3])
    reduce_second(units[1])
    reduce_third(units[0])
    reduce_second(units[2])
    old.line_step(2, ("xy",))
    old.line_step(1, ("d",))
    old.line_step(3, ("own",))
    reduce_third(units[1])
    reduce_second(units[3])
    for k in range(1, n_q):
        old.from_z(k)
        old.spread_y(k)
        old.core_copy(lat, k, 0, width)
    for k in range(n_q):
        old.spread_x(k)
    reduce_third(units[2])
    reduce_third(units[3])
    old.line_step(3, ("xy",))
    old.line_step(2, ("d",))
    for k in range(n_q):
        old.relay_y(k)
        old.relay_x(k)
    arrived(last_in, third_landed)
    square = jnp.zeros((rows, width), jnp.float32)
    for index, tap in enumerate(order):
        grad = mine[index, q]
        for k in range(n_q - 1):
            grad = grad + last_in[k, index].astype(jnp.float32)
        clipped[tap] = grad
        square = square + grad * grad
    square = jnp.sum(square)
    slot = 0
    for stage, peers in enumerate(([partner] + z_peers + z_twins, [x_peer, y_peer, d_peer])):
        norm_out[stage] = jnp.full(norm_out.shape[1:], square, jnp.float32)
        tiles = norm_in.at[pl.ds(slot, len(peers))]
        sent, landed_at = outgoing(tiles), landing()
        for index, target in enumerate(peers):
            send(norm_out.at[stage], norm_in.at[slot + index], target, sent, landed_at)
        arrived(tiles, landed_at)
        tile = norm_out[stage]
        for index in range(len(peers)):
            tile = tile + norm_in[slot + index]
        slot += len(peers)
        square = jnp.max(tile)
    one_load.wait()
    two_load.wait()
    square = jnp.full((1, 1), square, jnp.float32)
    clip_factor = jnp.minimum(1.0, max_norm / (jnp.sqrt(square) + norm_eps))

    @pl.loop(0, taps)
    def _(tap):
        scaled = clip_factor * clipped[tap]
        clipped[tap] = scaled
        moment = beta_one * one[tap] + (1.0 - beta_one) * scaled
        spread = beta_two * two[tap] + (1.0 - beta_two) * scaled * scaled
        new_one[tap] = moment
        new_two[tap] = spread
        first_hat = moment / (1.0 - beta_one**step_count)
        second_hat = spread / (1.0 - beta_two**step_count)
        updated = master[tap] - learn_rate * (
            first_hat / (jnp.sqrt(second_hat) + adam_eps) + decay_rate * master[tap]
        )
        new_master[tap] = updated
        w_new[tap, lat, q, core] = updated.astype(jnp.bfloat16)

    new = Gather(w_new, half, NEW_LINE_TAPS)
    new.line_start()
    new.line_start_y()
    new.start_z()
    new.spread_x(0)
    new.spread_y(0)
    new.core_copy(lat, 0, 0, width)
    old.line_step(3, ("d",))
    for step in range(4, n_q):
        old.line_step(step)
    for k in range(n_q):
        old.close(k)
    old.finish()
    cuts = [chunks * index // (n_q + 2) for index in range(n_q + 3)]
    input_pieces(cuts[0], cuts[1])
    new.line_cross()
    for k in range(1, n_q):
        input_pieces(cuts[k], cuts[k + 1])
        new.from_z(k)
        new.spread_x(k)
        new.spread_y(k)
        new.core_copy(lat, k, 0, width)
        new.relay_x(k - 1)
        new.relay_y(k - 1)
        if k == 1:
            new.line_far()
        new.line_step(k - 1 if k > 1 else n_q)
    input_pieces(cuts[n_q], cuts[n_q + 1])
    new.relay_x(n_q - 1)
    new.relay_y(n_q - 1)
    new.line_step(n_q - 1)
    input_pieces(cuts[n_q + 1], cuts[n_q + 2])
    for k in range(n_q):
        new.close(k)
    new.finish()

    for condition, copy in closing:
        if condition is None:
            copy.wait_send()
        else:
            @pl.when(condition)
            def _(copy=copy):
                copy.wait_send()

    assert used == [send_sem.shape[0], recv_sem.shape[0]]


def land(*refs):
    count = len(refs) // 2
    sources, targets, sem = refs[:count], refs[count : 2 * count], refs[-1]
    copies = [
        pltpu.make_async_copy(source, target, sem.at[index])
        for index, (source, target) in enumerate(zip(sources, targets))
    ]
    for copy in copies:
        copy.start()
    for copy in copies:
        copy.wait()


def landed(arrays):
    anywhere = pl.BlockSpec(memory_space=pl.ANY)
    return pl.pallas_call(
        land,
        out_shape=tuple(jax.ShapeDtypeStruct(a.shape, a.dtype) for a in arrays),
        in_specs=[anywhere] * len(arrays),
        out_specs=(anywhere,) * len(arrays),
        scratch_shapes=[pltpu.SemaphoreType.DMA((len(arrays),))],
        compiler_params=pltpu.CompilerParams(vmem_limit_bytes=1024 * 1024),
        name="land",
    )(*arrays)


def fused_step(up, act, master, one, two):
    n_lat, n_q = lax.axis_size("lat"), lax.axis_size("lon") // 2
    taps, rows, width = master.shape
    batch, cols, lat_rows, _ = up.shape
    group_rows = batch * lat_rows
    chunk = max(c for c in range(1, 17) if cols % c == 0)
    chunks = cols // chunk
    halo_rows = -(-chunk * batch // ROW_TILE) * ROW_TILE
    max_norm = math.sqrt(float(n_lat * n_q * 2 * taps * rows * width))
    bf16, f32 = jnp.bfloat16, jnp.float32
    shard = pltpu.VMEM(master.shape, f32)
    whole = (taps, n_lat, n_q, 2, rows, width)
    lat_block = (taps, n_q, rows, width)
    vmem, hbm = (pl.BlockSpec(memory_space=m) for m in (pltpu.VMEM, pltpu.HBM))
    peers = 2 * n_q + n_lat - 2
    sends, arrivals = 28 + 4 * (n_q - 1), 38 + 9 * n_q + 12 * (n_q - 1)
    return pl.pallas_call(
        functools.partial(whole_step, n_lat, n_q, max_norm),
        out_shape=(
            pltpu.VMEM(up.shape, bf16), pltpu.VMEM(whole, bf16), shard, shard, shard, shard,
        ),
        in_specs=[hbm] * 5,
        out_specs=(vmem,) * 6,
        scratch_shapes=[
            pltpu.VMEM(master.shape, f32),
            pltpu.VMEM(master.shape, f32),
            pltpu.VMEM(master.shape, f32),
            pltpu.VMEM((cols, batch, lat_rows, width), bf16),
            pltpu.VMEM((cols, batch, lat_rows, width), bf16),
            pltpu.VMEM((cols * group_rows, width), bf16),
            pltpu.VMEM((3, cols + 2, group_rows, width), bf16),
            pltpu.VMEM((2, chunks, halo_rows, width), bf16),
            pltpu.VMEM((2, chunks, halo_rows, width), bf16),
            pltpu.VMEM((chunks // 2, halo_rows, width), bf16),
            pltpu.VMEM(whole, bf16),
            pltpu.VMEM(whole, f32),
            pltpu.VMEM((taps, n_lat, n_q, rows, width), f32),
            pltpu.VMEM(lat_block, f32),
            pltpu.VMEM(lat_block, f32),
            pltpu.VMEM((taps, 2, n_q, rows, width), bf16),
            pltpu.VMEM((taps, 2, n_q, rows, width), bf16),
            pltpu.VMEM(lat_block, bf16),
            pltpu.VMEM(lat_block, bf16),
            pltpu.VMEM((n_q - 1, taps, rows, width), bf16),
            pltpu.VMEM((n_q - 1, taps, rows, width), bf16),
            pltpu.VMEM((3, 8, LANE_TILE), f32),
            pltpu.VMEM((peers, 8, LANE_TILE), f32),
            pltpu.SemaphoreType.DMA((2 * batch + 3,)),
            pltpu.SemaphoreType.DMA((sends,)),
            pltpu.SemaphoreType.DMA((arrivals,)),
        ],
        compiler_params=pltpu.CompilerParams(
            collective_id=2, has_side_effects=True, vmem_limit_bytes=48 * 1024 * 1024
        ),
        name="whole_step",
    )(up, act, master, one, two)


def takes_fused(activations, master):
    n_lat, n_q = lax.axis_size("lat"), lax.axis_size("lon") // 2
    batch, lat_rows, cols, _ = activations.shape
    return (
        n_lat == 4 and n_q & (n_q - 1) == 0 and n_q > 1 and master.shape[0] % ROW_TILE == 0
        and (batch * lat_rows) % ROW_TILE == 0 and cols % 2 == 0
        and master.shape[2] % (2 * LANE_TILE) == 0 and master.shape[1] == 9
    )


def per_device(activations, upstream, master, moment_one, moment_two):
    if not takes_fused(activations, master):
        return per_device_general(activations, upstream, master, moment_one, moment_two)

    def by_col(field):
        return jnp.transpose(field, (0, 2, 1, 3))

    def by_tap(array):
        return jnp.transpose(array, (1, 0, 2))

    input_grad, gathered, new_master, new_one, new_two, clipped = landed(fused_step(
        by_col(upstream), by_col(activations), by_tap(master), by_tap(moment_one),
        by_tap(moment_two),
    ))
    new_weights = by_tap(gathered.reshape(gathered.shape[0], -1, gathered.shape[-1]))
    return (
        by_col(input_grad), new_weights, by_tap(new_master), by_tap(new_one), by_tap(new_two),
        by_tap(clipped),
    )


def per_device_general(activations, upstream, master, moment_one, moment_two):
    lat_rows = activations.shape[1]
    lon_cols = activations.shape[2]
    grad_flat = upstream.reshape(-1, upstream.shape[3])
    old_weights = master[:, ::-1].astype(jnp.bfloat16)
    old_full = lax.all_gather(old_weights, ("lat", "lon"), axis=0, tiled=True)
    act_wide, grad_wide = widened((activations, upstream))
    term_maker = input_taps(act_wide, grad_flat, lat_rows, lon_cols)
    partial = term_maker(jnp.int32(0), activations.shape[3])

    def by_tap(array):
        return jnp.transpose(array, (1, 0, 2))

    gathered, new_master, new_one, new_two, clipped = fused_update(
        by_tap(partial), by_tap(master), by_tap(moment_one), by_tap(moment_two)
    )
    new_weights = jnp.transpose(gathered, (2, 1, 0, 4, 3, 5)).reshape(
        activations.shape[3], gathered.shape[3], gathered.shape[5]
    )
    old_full, new_one = lax.optimization_barrier((old_full, new_one))
    input_grad = lax.conv_general_dilated(
        grad_wide,
        old_full.reshape(old_full.shape[0], 3, 3, old_full.shape[2]),
        (1, 1),
        "VALID",
        dimension_numbers=("NHWC", "OHWI", "NHWC"),
        preferred_element_type=jnp.float32,
    ).astype(jnp.bfloat16)
    return (
        input_grad, new_weights, by_tap(new_master), by_tap(new_one), by_tap(new_two),
        by_tap(clipped),
    )


def solution(mesh):
    in_specs = (
        P(None, "lat", "lon", None),
        P(None, "lat", "lon", None),
        P(("lat", "lon"), None, None),
        P(("lat", "lon"), None, None),
        P(("lat", "lon"), None, None),
    )
    out_specs = (
        P(None, "lat", "lon", None),
        P(),
        P(("lat", "lon"), None, None),
        P(("lat", "lon"), None, None),
        P(("lat", "lon"), None, None),
        P(("lat", "lon"), None, None),
    )
    return jax.shard_map(
        per_device, mesh=mesh, in_specs=in_specs, out_specs=out_specs, check_vma=False
    )
```
